32 devices in a mesh: seq: 16 (over z, y, core), head: 2 (over x).
Axes of the slice: x: 2, y: 2, z: 4, core: 2. Of those that a mesh axis runs over, the one named last changes fastest.
Arguments:
- query: bfloat16 [1024, 5120], P('seq', 'head'), may hold values from -3 to 3
- query_offset: int32 [1024], P('seq'), may hold values from 0 to 255
- attn_out: bfloat16 [1024, 5120], P('seq', 'head'), may hold values from -3 to 3
- out_grad: bfloat16 [1024, 5120], P('seq', 'head'), may hold values from -24 to 24
- log_norm: float32 [40, 1024], P('head', 'seq'), may hold values from 4 to 6
- keys: bfloat16 [4096, 5120], P('seq', 'head'), may hold values from -6 to 6
- values: bfloat16 [4096, 5120], P('seq', 'head'), may hold values from -6 to 6
Outputs:
- key_grad: bfloat16 [4096, 5120], P('seq', 'head')
- value_grad: bfloat16 [4096, 5120], P('seq', 'head')
- query_grad: bfloat16 [1024, 5120], P(('seq', 'head'))
The draws below stay inside these ranges and needn't reach their ends.
All inputs are finite; a program needn't handle non-finite values.
Results may differ from the reference program's by a relative error of at most 0.0051.
Values may be sent and summed in bfloat16 or wider, within the bound.
A program may use at most 64 MiB of HBM per device.

```python
import math
import jax
import jax.numpy as jnp
from jax import lax

HEADS = 40
DH = 128
KB = 256
QB = 64
STEPS = 4
F = 5120
NQ = 1024
NK = 4096
N_SEQ = 16


def plant(array, key, smallest, largest):
    longest = array.shape.index(max(array.shape))
    spots = []
    for shift in (0, 1):
        where = [jax.random.randint(jax.random.fold_in(key, axis), (), 0, length) for axis, length in enumerate(array.shape)]
        where[longest] = (where[longest] + shift) % array.shape[longest]
        spots.append(tuple(where))
    return array.at[spots[0]].set(smallest).at[spots[1]].set(largest)


def block_scale(rng, extent, pieces, smallest, largest):
    def one(dim, blocks):
        heights = jax.random.uniform(jax.random.fold_in(jax.random.fold_in(rng, 6), dim), (blocks,), jnp.float32, smallest / len(pieces), largest / len(pieces))
        return jnp.repeat(jnp.exp(heights), extent[dim] // blocks).reshape((-1,) + (1,) * (len(extent) - dim - 1))

    factor_of = one(*pieces[0])
    for cut in pieces[1:]:
        factor_of = factor_of * one(*cut)
    return factor_of


def centred(own_key, shape, scale, limit, pieces=(), kind=jnp.bfloat16):
    entries = jax.random.normal(own_key, shape, jnp.float32) * scale
    if len(pieces) > 0:
        entries = block_scale(own_key, shape, pieces, -0.22, 0.18) * entries
    return jnp.clip(entries, min=-limit, max=limit).astype(kind)


def setup_inputs(seed: int = 0) -> dict:
    seeds = jax.random.split(jax.random.key(seed), 8)
    return {
        "query": centred(seeds[0], (NQ, F), 0.5, 3.0, ((0, 16), (1, 2))),
        "query_offset": plant(jax.random.randint(seeds[1], (NQ,), 0, KB), jax.random.fold_in(seeds[1], 1), 0, KB - 1).astype(jnp.int32),
        "attn_out": centred(seeds[2], (NQ, F), 0.5, 3.0, ((0, 16), (1, 2))),
        "out_grad": centred(seeds[3], (NQ, F), 4.0, 24.0, ((0, 16), (1, 2))),
        "log_norm": jnp.clip(4.0 + 2.0 * jax.random.uniform(seeds[4], (HEADS, NQ), jnp.float32) ** block_scale(seeds[4], (HEADS, NQ), ((0, 2), (1, 16)), -0.2, 0.2), 4.0, 6.0),
        "keys": centred(seeds[5], (NK, F), 1.0, 6.0, ((0, 16), (1, 2))),
        "values": centred(seeds[6], (NK, F), 1.0, 6.0, ((0, 16), (1, 2))),
    }


def reference(query, query_offset, attn_out, out_grad, log_norm, keys, values):
    scale = 1.0 / math.sqrt(DH)
    extra = (STEPS - 1) * QB
    span = STEPS * QB
    delta = lax.optimization_barrier(jnp.sum((out_grad.astype(jnp.float32) * attn_out.astype(jnp.float32)).reshape(NQ, HEADS, DH), axis=2)).T
    query_pad = jnp.concatenate([query.astype(jnp.float32), jnp.zeros((extra, F), jnp.float32)], axis=0)
    grad_pad = jnp.concatenate([out_grad.astype(jnp.float32), jnp.zeros((extra, F), jnp.float32)], axis=0)
    offset_pad = jnp.concatenate([query_offset.astype(jnp.int32), jnp.zeros((extra,), jnp.int32)], axis=0)
    norm_pad = jnp.concatenate([log_norm, jnp.zeros((HEADS, extra), log_norm.dtype)], axis=1)
    delta_pad = jnp.concatenate([delta, jnp.zeros((HEADS, extra), delta.dtype)], axis=1)

    def one_block(summed, block_index):
        start = (block_index * QB).astype(jnp.int32)
        key_start = (block_index * KB).astype(jnp.int32)
        query_heads = lax.dynamic_slice_in_dim(query_pad, start, span, 0).reshape(span, HEADS, DH)
        grad_heads = lax.dynamic_slice_in_dim(grad_pad, start, span, 0).reshape(span, HEADS, DH)
        offsets = lax.dynamic_slice_in_dim(offset_pad, start, span, 0)
        norms = lax.dynamic_slice_in_dim(norm_pad, start, span, 1)
        deltas = lax.dynamic_slice_in_dim(delta_pad, start, span, 1)
        key_heads = lax.dynamic_slice_in_dim(keys, key_start, KB, 0).astype(jnp.float32).reshape(KB, HEADS, DH)
        value_heads = lax.dynamic_slice_in_dim(values, key_start, KB, 0).astype(jnp.float32).reshape(KB, HEADS, DH)
        owner = block_index + jnp.arange(span, dtype=jnp.int32) // QB
        query_pos = owner * KB + offsets
        key_pos = block_index * KB + jnp.arange(KB, dtype=jnp.int32)
        allowed = (owner < N_SEQ)[:, None] & (key_pos[None, :] <= query_pos[:, None])
        scores = jnp.einsum('qhd,khd->hqk', query_heads, key_heads) * scale
        weights = jnp.where(allowed[None], jnp.exp(scores - norms[:, :, None]), 0.0)
        weights_low = lax.optimization_barrier(weights.astype(jnp.bfloat16)).astype(jnp.float32)
        value_part = jnp.einsum('hqk,qhd->khd', weights_low, grad_heads).reshape(KB, F)
        weight_grad = jnp.einsum('qhd,khd->hqk', grad_heads, value_heads)
        score_grad = weights * (weight_grad - deltas[:, :, None]) * scale
        score_low = lax.optimization_barrier(score_grad.astype(jnp.bfloat16)).astype(jnp.float32)
        query_part = jnp.einsum('hqk,khd->qhd', score_low, key_heads).reshape(span, F)
        key_part = jnp.einsum('hqk,qhd->khd', score_low, query_heads).reshape(KB, F)
        current = lax.dynamic_slice_in_dim(summed, start, span, 0)
        summed = lax.dynamic_update_slice_in_dim(summed, current + query_part, start, 0)
        return (summed, (key_part.astype(jnp.bfloat16), value_part.astype(jnp.bfloat16)))
    summed = jnp.zeros((NQ + extra, F), jnp.float32)
    summed, (key_parts, value_parts) = lax.scan(one_block, summed, jnp.arange(N_SEQ, dtype=jnp.int32))
    return (key_parts.reshape(NK, F), value_parts.reshape(NK, F), summed[:NQ].astype(jnp.bfloat16))
```

```python
import functools
import math

import jax
import jax.numpy as jnp
from jax import lax
from jax.experimental import pallas as pl
from jax.experimental.pallas import tpu as pltpu
from jax.sharding import PartitionSpec as P

STEPS = 4
HEADS_PER_CHUNK = 2
LAG0 = 1
LAG1 = 1
WAIT0 = 5
RATE0 = 2
LATE = 7
AHEAD = 2
F32 = jnp.float32
BF16 = jnp.bfloat16


def dot(a, b, ca, cb):
    return lax.dot_general(a, b, (((ca,), (cb,)), ((), ())), preferred_element_type=F32)


def kernel(
    dims, q_hbm, off_hbm, o_hbm, do_hbm, ln_hbm, k_hbm, v_hbm,
    kgb, vgb, outb,
    x, via, kb, vb, ob, lnb, offb, st, lse, dlt, offrow, own, part, got, fin,
    load_sem, kv_sem, small_sem, xs, xr, ss, sr, ps, pr, fs, fr,
):
    n, hn, heads, hc, dh, qb, kbr = dims
    chunks = heads // hc
    w = hc * dh
    feats = heads * dh
    rows_out = qb // hn
    scale = 1.0 / math.sqrt(dh)
    me = lax.axis_index("seq")
    hd = lax.axis_index("head")
    k = lax.rem(me, 2)
    partner = me + 1 - 2 * k
    oa = 1 + 2 * k
    oc = 3 - 2 * k
    quad = lax.rem(me, 4)
    q0, q1, q2, q3 = (quad == i for i in range(4))
    odd = k == 1
    lower = me >= 4
    has2 = me + 2 < n
    hasa = me + oa < n
    to2 = me >= 2
    toc = me >= oc

    def rows(o):
        return pl.ds(pl.multiple_of(o * qb, qb), qb)

    def cols(g):
        return pl.ds(pl.multiple_of(g * w, w), w)

    def load_q(g):
        return pltpu.make_async_copy(q_hbm.at[:, cols(g)], x.at[g, 0, pl.ds(0, qb)], load_sem.at[0, g])

    def load_do(g):
        return pltpu.make_async_copy(do_hbm.at[:, cols(g)], x.at[g, 1, pl.ds(0, qb)], load_sem.at[1, g])

    def load_k(g):
        return pltpu.make_async_copy(k_hbm.at[:, cols(g)], kb.at[g], kv_sem.at[0, g])

    def load_v(g):
        return pltpu.make_async_copy(v_hbm.at[:, cols(g)], vb.at[g], kv_sem.at[1, g])

    load_o = pltpu.make_async_copy(o_hbm, ob, small_sem.at[0])
    load_ln = pltpu.make_async_copy(ln_hbm, lnb, small_sem.at[1])
    load_off = pltpu.make_async_copy(off_hbm, offb, small_sem.at[2])

    def remote(src, dst, send, recv, target):
        return pltpu.make_async_remote_copy(
            src_ref=src, dst_ref=dst, send_sem=send, recv_sem=recv,
            device_id={"seq": target}, device_id_type=pl.DeviceIdType.MESH,
        )

    def mine(g):
        return x.at[g, :, pl.ds(0, qb)]

    def slot(g, o):
        return x.at[g, :, rows(o)]

    def x_two(g):
        return remote(mine(g), slot(g, 2), xs.at[0, g], xr.at[0, g], me - 2)

    def x_chip(g):
        return remote(mine(g), slot(g, 1), xs.at[1, g], xr.at[1, g], me - 1)

    def x_three(g):
        return remote(mine(g), slot(g, 3), xs.at[1, g], xr.at[1, g], me - 3)

    def x_side(g):
        return remote(mine(g), via.at[g], xs.at[0, g], xr.at[3, g], me + 3)

    def via_down(g):
        return remote(via.at[g], slot(g, 2), xs.at[3, g], xr.at[0, g], me - 5)

    def x_relay(g):
        return remote(slot(g, 2), slot(g, oa), xs.at[2, g], xr.at[2, g], partner)

    def st_send(o):
        return remote(st.at[0], st.at[o], ss.at[o - 1], sr.at[o - 1], me - o)

    def p_partner(g):
        return remote(part.at[g, rows(oc)], got.at[0, g], ps.at[0, g], pr.at[0, g], partner)

    def p_ahead(g):
        return remote(part.at[g, rows(oa)], got.at[1, g], ps.at[1, g], pr.at[1, g], me + oa)

    def p_two(g):
        return remote(part.at[g, rows(2)], got.at[2, g], ps.at[2, g], pr.at[2, g], me + 2)

    def f_send(g, d):
        peer = lax.rem(hd + d, hn)
        return pltpu.make_async_remote_copy(
            src_ref=fin.at[g, pl.ds(pl.multiple_of(peer * rows_out, rows_out), rows_out)],
            dst_ref=outb.at[:, pl.ds(pl.multiple_of(hd * feats + g * w, w), w)],
            send_sem=fs.at[d - 1, g], recv_sem=fr.at[d - 1, g],
            device_id={"head": peer}, device_id_type=pl.DeviceIdType.MESH,
        )

    @pl.loop(0, chunks)
    def _(g):
        load_do(g).start()
        load_q(g).start()

    load_o.start()
    load_ln.start()
    load_off.start()

    barrier = pltpu.get_barrier_semaphore()

    def greet(cond, target):
        @pl.when(cond)
        def _():
            pl.semaphore_signal(barrier, inc=1, device_id={"seq": target}, device_id_type=pl.DeviceIdType.MESH)

        return cond.astype(jnp.int32)

    peers = hn - 1
    for d in (1, 2, 3, 5):
        peers = peers + greet(me >= d, me - d) + greet(me + d < n, me + d)
    for d in range(1, hn):
        pl.semaphore_signal(
            barrier, inc=1, device_id={"head": lax.rem(hd + d, hn)}, device_id_type=pl.DeviceIdType.MESH
        )

    load_o.wait()
    load_ln.wait()

    @pl.loop(0, chunks)
    def _(g):
        load_q(g).wait()
        load_do(g).wait()

    st[0, :, 0:qb] = lnb[...]
    eye = lax.broadcasted_iota(jnp.int32, (qb, qb), 0) == lax.broadcasted_iota(jnp.int32, (qb, qb), 1)
    for h in range(heads):
        oh = ob[:, h * dh:(h + 1) * dh]
        doh = x[h // hc, 1, 0:qb, h % hc * dh:(h % hc + 1) * dh]
        t = dot(oh, doh, 1, 1)
        st[0, h:h + 1, qb:2 * qb] = jnp.sum(jnp.where(eye, t, 0.0), axis=0, keepdims=True)

    pl.semaphore_wait(barrier, peers)

    def send_x(g):
        pl.when(q2 | q3 | (q1 & lower))(lambda: x_two(g).start())
        pl.when(q0 & lower)(lambda: x_side(g).start())
        pl.when(odd)(lambda: x_chip(g).start())
        pl.when((q0 | q2) & lower)(lambda: x_three(g).start())

    send_x(0)

    for o in range(1, STEPS):
        pl.when(me >= o)(lambda o=o: st_send(o).start())

    @pl.loop(1, chunks)
    def _(g):
        send_x(g)

    @pl.loop(0, chunks)
    def _(g):
        load_k(g).start()
        load_v(g).start()

    for o in range(1, STEPS):

        @pl.when(me + o >= n)
        def _(o=o):
            @pl.loop(0, chunks)
            def _(g):
                for i in range(2):
                    x[g, i, rows(o), :] = jnp.zeros((qb, w), BF16)

            st[o] = jnp.zeros_like(st[o])

    load_off.wait()
    offrow[...] = jnp.full(offrow.shape, kbr, jnp.int32)
    offrow[:, 0:qb] = offb[...]

    def forward(g):
        @pl.when(q3 & lower)
        def _():
            x_side(g).wait_recv()
            via_down(g).start()

    def relay(g):
        @pl.when(has2)
        def _():
            x_two(g).wait_recv()
            x_relay(g).start()

    def compute(g):
        @pl.when(hasa)
        def _():
            x_chip(g).wait_recv()

        pl.when(has2)(lambda: x_relay(g).wait_recv())
        load_k(g).wait()
        load_v(g).wait()
        allowed = lax.broadcasted_iota(jnp.int32, (kbr, STEPS * qb), 0) <= offrow[...]
        for h in range(hc):
            c = slice(h * dh, (h + 1) * dh)
            qh = x[g, 0, :, c]
            doh = x[g, 1, :, c]
            kh = kb[g, :, c]
            vh = vb[g, :, c]
            row = pl.ds(g * hc + h, 1)
            s = dot(kh, qh, 1, 1) * scale - lse[row, :]
            p = jnp.where(allowed, jnp.exp(s), 0.0)
            dp = dot(vh, doh, 1, 1)
            ds = (p * (dp - dlt[row, :]) * scale).astype(BF16)
            out = pl.ds(pl.multiple_of(g * w + h * dh, dh), dh)
            vgb[:, out] = dot(p.astype(BF16), doh, 1, 0).astype(BF16)
            kgb[:, out] = dot(ds, qh, 1, 0).astype(BF16)
            dq = dot(ds, kh, 0, 0)
            own[g, :, c] = dq
            part[g, :, c] = dq.astype(BF16)
        pl.when(has2)(lambda: p_partner(g).start())
        pl.when(hasa)(lambda: p_ahead(g).start())

    def combine(g):
        @pl.when(has2)
        def _():
            p_partner(g).wait_recv()
            both = own[g, 2 * qb:3 * qb, :] + got[0, g].astype(F32)
            part[g, 2 * qb:3 * qb, :] = both.astype(BF16)
            p_two(g).start()

    def finish(g):
        @pl.when(to2)
        def _():
            p_two(g).wait_recv()
            own[g, 0:qb, :] = own[g, 0:qb, :] + got[2, g].astype(F32)

        @pl.when(toc)
        def _():
            p_ahead(g).wait_recv()
            own[g, 0:qb, :] = own[g, 0:qb, :] + got[1, g].astype(F32)

        fin[g] = own[g, 0:qb, :].astype(BF16)
        for d in range(1, hn):
            f_send(g, d).start()
        outb[:, pl.ds(pl.multiple_of(hd * feats + g * w, w), w)] = fin[
            g, pl.ds(pl.multiple_of(hd * rows_out, rows_out), rows_out), :
        ]

    for g in range(min(AHEAD, chunks)):
        forward(g)
    relay(0)

    for o in range(1, STEPS):
        pl.when(me + o < n)(lambda o=o: st_send(o).wait_recv())
    for o in range(STEPS):
        lse[:, o * qb:(o + 1) * qb] = st[o, :, 0:qb]
        dlt[:, o * qb:(o + 1) * qb] = st[o, :, qb:2 * qb]

    def sent(t):
        below = jnp.clip((t - WAIT0) * RATE0, 0, t - LAG0)
        return jnp.clip(jnp.where((quad < 2) & (me + 4 < n), below, t - LAG1), 0, chunks)

    def done(t):
        return jnp.clip(t - jnp.where(me < 2, 1, LATE), 0, chunks)

    @pl.loop(1, chunks + 1)
    def _(t):
        pl.when(t + AHEAD - 1 < chunks)(lambda: forward(t + AHEAD - 1))
        pl.when(t < chunks)(lambda: relay(t))
        compute(t - 1)

        @pl.loop(sent(t - 1), sent(t))
        def _(g):
            combine(g)

        @pl.loop(done(t - 1), done(t))
        def _(g):
            finish(g)

    @pl.loop(sent(chunks), chunks)
    def _(g):
        combine(g)

    @pl.loop(done(chunks), chunks)
    def _(g):
        finish(g)

    @pl.loop(0, chunks)
    def _(g):
        pl.when(q2 | q3 | lower)(lambda: x_two(g).wait_send())
        pl.when(odd | lower)(lambda: x_chip(g).wait_send())
        pl.when(q3 & lower)(lambda: via_down(g).wait_send())

        @pl.when(has2)
        def _():
            x_relay(g).wait_send()
            p_partner(g).wait_send()
            p_two(g).wait_send()

        pl.when(hasa)(lambda: p_ahead(g).wait_send())

    for o in range(1, STEPS):
        pl.when(me >= o)(lambda o=o: st_send(o).wait_send())

    @pl.loop(0, chunks)
    def _(g):
        for d in range(1, hn):
            f_send(g, d).wait()


def write_out(kgb, vgb, outb, kg_hbm, vg_hbm, qg_hbm, sem):
    copies = [
        pltpu.make_async_copy(src, dst, sem.at[i])
        for i, (src, dst) in enumerate(((kgb, kg_hbm), (vgb, vg_hbm), (outb, qg_hbm)))
    ]
    for copy in copies:
        copy.start()
    for copy in copies:
        copy.wait()


def per_device(query, query_offset, attn_out, out_grad, log_norm, keys, values):
    n = lax.axis_size("seq")
    hn = lax.axis_size("head")
    heads = log_norm.shape[0]
    qb, feats = query.shape
    kbr = keys.shape[0]
    dh = feats // heads
    hc = HEADS_PER_CHUNK
    while heads % hc:
        hc -= 1
    chunks = heads // hc
    w = hc * dh
    dims = (n, hn, heads, hc, dh, qb, kbr)
    span = STEPS * qb
    dma = pltpu.SemaphoreType.DMA
    args = (query, query_offset.reshape(1, qb), attn_out, out_grad, log_norm, keys, values)
    outs = (
        jax.ShapeDtypeStruct((kbr, feats), BF16),
        jax.ShapeDtypeStruct((kbr, feats), BF16),
        jax.ShapeDtypeStruct((qb // hn, feats * hn), BF16),
    )
    grads = pl.pallas_call(
        functools.partial(kernel, dims),
        out_shape=tuple(pltpu.VMEM(o.shape, o.dtype) for o in outs),
        in_specs=[pl.BlockSpec(memory_space=pl.ANY)] * 7,
        out_specs=tuple([pl.BlockSpec(memory_space=pltpu.VMEM)] * 3),
        scratch_shapes=[
            pltpu.VMEM((chunks, 2, span, w), BF16),
            pltpu.VMEM((chunks, 2, qb, w), BF16),
            pltpu.VMEM((chunks, kbr, w), BF16),
            pltpu.VMEM((chunks, kbr, w), BF16),
            pltpu.VMEM((qb, feats), BF16),
            pltpu.VMEM((heads, qb), F32),
            pltpu.VMEM((1, qb), jnp.int32),
            pltpu.VMEM((STEPS, heads, 2 * qb), F32),
            pltpu.VMEM((heads, span), F32),
            pltpu.VMEM((heads, span), F32),
            pltpu.VMEM((1, span), jnp.int32),
            pltpu.VMEM((chunks, span, w), F32),
            pltpu.VMEM((chunks, span, w), BF16),
            pltpu.VMEM((3, chunks, qb, w), BF16),
            pltpu.VMEM((chunks, qb, w), BF16),
            dma((2, chunks)), dma((2, chunks)), dma((3,)),
            dma((4, chunks)), dma((4, chunks)), dma((3,)), dma((3,)),
            dma((3, chunks)), dma((3, chunks)),
            dma((max(hn - 1, 1), chunks)), dma((max(hn - 1, 1), chunks)),
        ],
        compiler_params=pltpu.CompilerParams(
            collective_id=0, has_side_effects=True, vmem_limit_bytes=40 * 1024 * 1024
        ),
    )(*[pltpu.with_memory_space_constraint(a, pltpu.HBM) for a in args])
    return pl.pallas_call(
        write_out,
        out_shape=outs,
        in_specs=[pl.BlockSpec(memory_space=pltpu.VMEM)] * 3,
        out_specs=tuple([pl.BlockSpec(memory_space=pl.ANY)] * 3),
        scratch_shapes=[dma((3,))],
        compiler_params=pltpu.CompilerParams(vmem_limit_bytes=16 * 1024 * 1024),
    )(*grads)


def solution(mesh):
    in_specs = (
        P("seq", "head"),
        P("seq"),
        P("seq", "head"),
        P("seq", "head"),
        P("head", "seq"),
        P("seq", "head"),
        P("seq", "head"),
    )
    out_specs = (P("seq", "head"), P("seq", "head"), P(("seq", "head"), None))
    return jax.shard_map(
        per_device, mesh=mesh, in_specs=in_specs, out_specs=out_specs, check_vma=False
    )
```

```python
import functools
import math

import jax
import jax.numpy as jnp
from jax import lax
from jax.experimental import pallas as pl
from jax.experimental.pallas import tpu as pltpu
from jax.sharding import PartitionSpec as P

STEPS = 4
HEADS_PER_CHUNK = 2
LAG0 = 1
LAG1 = 1
WAIT0 = 5
RATE0 = 2
FROM = 2
UPTO = 8
AHEAD = 3
F32 = jnp.float32
BF16 = jnp.bfloat16


def dot(a, b, ca, cb):
    return lax.dot_general(a, b, (((ca,), (cb,)), ((), ())), preferred_element_type=F32)


def kernel(
    dims, q_hbm, off_hbm, o_hbm, do_hbm, ln_hbm, k_hbm, v_hbm,
    kgb, vgb, outb,
    x, via, kb, vb, ob, lnb, offb, st, lse, dlt, offrow, own, part, got, mate,
    load_sem, kv_sem, small_sem, xs, xr, ss, sr, ps, pr, rsnd, rrcv,
):
    n, hn, heads, hc, dh, qb, kbr = dims
    chunks = heads // hc
    w = hc * dh
    feats = heads * dh
    rows_out = qb // hn
    scale = 1.0 / math.sqrt(dh)
    me = lax.axis_index("seq")
    hd = lax.axis_index("head")
    k = lax.rem(me, 2)
    partner = me + 1 - 2 * k
    oa = 1 + 2 * k
    oc = 3 - 2 * k
    quad = lax.rem(me, 4)
    q0, q1, q2, q3 = (quad == i for i in range(4))
    odd = k == 1
    lower = me >= 4
    has2 = me + 2 < n
    hasa = me + oa < n
    to2 = me >= 2
    toc = me >= oc

    def rows(o):
        return pl.ds(pl.multiple_of(o * qb, qb), qb)

    def cols(g):
        return pl.ds(pl.multiple_of(g * w, w), w)

    def load_q(g):
        return pltpu.make_async_copy(q_hbm.at[:, cols(g)], x.at[g, 0, pl.ds(0, qb)], load_sem.at[0, g])

    def load_do(g):
        return pltpu.make_async_copy(do_hbm.at[:, cols(g)], x.at[g, 1, pl.ds(0, qb)], load_sem.at[1, g])

    def load_k(g):
        return pltpu.make_async_copy(k_hbm.at[:, cols(g)], kb.at[g], kv_sem.at[0, g])

    def load_v(g):
        return pltpu.make_async_copy(v_hbm.at[:, cols(g)], vb.at[g], kv_sem.at[1, g])

    load_o = pltpu.make_async_copy(o_hbm, ob, small_sem.at[0])
    load_ln = pltpu.make_async_copy(ln_hbm, lnb, small_sem.at[1])
    load_off = pltpu.make_async_copy(off_hbm, offb, small_sem.at[2])

    def remote(src, dst, send, recv, target):
        return pltpu.make_async_remote_copy(
            src_ref=src, dst_ref=dst, send_sem=send, recv_sem=recv,
            device_id={"seq": target}, device_id_type=pl.DeviceIdType.MESH,
        )

    def mine(g):
        return x.at[g, :, pl.ds(0, qb)]

    def slot(g, o):
        return x.at[g, :, rows(o)]

    def x_two(g):
        return remote(mine(g), slot(g, 2), xs.at[0, g], xr.at[0, g], me - 2)

    def x_chip(g):
        return remote(mine(g), slot(g, 1), xs.at[1, g], xr.at[1, g], me - 1)

    def x_three(g):
        return remote(mine(g), slot(g, 3), xs.at[1, g], xr.at[1, g], me - 3)

    def x_side(g):
        return remote(mine(g), via.at[g], xs.at[0, g], xr.at[3, g], me + 3)

    def via_down(g):
        return remote(via.at[g], slot(g, 2), xs.at[3, g], xr.at[0, g], me - 5)

    def relayed(g):
        return (g >= chunks * FROM // 10) & (g < chunks * UPTO // 10)

    def x_relay(g):
        return remote(slot(g, 2), slot(g, oa), xs.at[2, g], xr.at[2, g], partner)

    def st_send(o):
        return remote(st.at[0], st.at[o], ss.at[o - 1], sr.at[o - 1], me - o)

    def p_partner(g):
        return remote(part.at[g, rows(oc)], got.at[g], ps.at[g], pr.at[g], partner)

    def piece(hs):
        return pl.multiple_of(hs * rows_out, rows_out)

    def back(kind, g, d, ahead, o):
        peer = lax.rem(hd + d, hn)
        return pltpu.make_async_remote_copy(
            src_ref=part.at[g, pl.ds(pl.multiple_of(o * qb, qb) + piece(peer), rows_out)],
            dst_ref=mate.at[kind, hd, g], send_sem=rsnd.at[kind, d, g], recv_sem=rrcv.at[kind, hd, g],
            device_id={"seq": me + ahead, "head": peer}, device_id_type=pl.DeviceIdType.MESH,
        )

    def p_own(g, d):
        return back(0, g, d, 0, 0)

    def p_ahead(g, d):
        return back(1, g, d, oa, oa)

    def p_two(g, d):
        return back(2, g, d, 2, 2)

    def arrived(kind, g, hs):
        return pltpu.make_async_copy(mate.at[kind, hs, g], mate.at[kind, hs, g], rrcv.at[kind, hs, g])

    @pl.loop(0, chunks)
    def _(g):
        load_do(g).start()
        load_q(g).start()

    load_o.start()
    load_ln.start()
    load_off.start()

    barrier = pltpu.get_barrier_semaphore()

    def greet(cond, ahead, d=0):
        @pl.when(cond)
        def _():
            pl.semaphore_signal(
                barrier, inc=1, device_id={"seq": me + ahead, "head": lax.rem(hd + d, hn)},
                device_id_type=pl.DeviceIdType.MESH,
            )

        return cond.astype(jnp.int32)

    peers = 0
    for o in range(1, STEPS):
        peers = peers + greet(me >= o, -o) + greet(me + o < n, o)
    peers = peers + greet(q3 & lower, -5) + greet(q2 & (me + 5 < n), 5)
    for d in range(1, hn):
        peers = peers + greet(me >= 0, 0, d)
        peers = peers + greet(to2, -2, d) + greet(has2, 2, d) + greet(toc, -oc, d) + greet(hasa, oa, d)

    load_o.wait()
    load_ln.wait()

    @pl.loop(0, chunks)
    def _(g):
        load_q(g).wait()
        load_do(g).wait()

    st[0, :, 0:qb] = lnb[...]
    eye = lax.broadcasted_iota(jnp.int32, (qb, qb), 0) == lax.broadcasted_iota(jnp.int32, (qb, qb), 1)
    for h in range(heads):
        oh = ob[:, h * dh:(h + 1) * dh]
        doh = x[h // hc, 1, 0:qb, h % hc * dh:(h % hc + 1) * dh]
        t = dot(oh, doh, 1, 1)
        st[0, h:h + 1, qb:2 * qb] = jnp.sum(jnp.where(eye, t, 0.0), axis=0, keepdims=True)

    pl.semaphore_wait(barrier, peers)

    def send_x(g):
        pl.when(q2 | q3 | (lower & (q1 | (q0 & jnp.logical_not(relayed(g))))))(lambda: x_two(g).start())
        pl.when(q0 & lower & relayed(g))(lambda: x_side(g).start())
        pl.when(odd)(lambda: x_chip(g).start())
        pl.when((q0 | q2) & lower)(lambda: x_three(g).start())

    send_x(0)

    for o in range(1, STEPS):
        pl.when(me >= o)(lambda o=o: st_send(o).start())

    @pl.loop(1, chunks)
    def _(g):
        send_x(g)

    @pl.loop(0, chunks)
    def _(g):
        load_k(g).start()
        load_v(g).start()

    for o in range(1, STEPS):

        @pl.when(me + o >= n)
        def _(o=o):
            @pl.loop(0, chunks)
            def _(g):
                for i in range(2):
                    x[g, i, rows(o), :] = jnp.zeros((qb, w), BF16)

            st[o] = jnp.zeros_like(st[o])

    load_off.wait()
    offrow[...] = jnp.full(offrow.shape, kbr, jnp.int32)
    offrow[:, 0:qb] = offb[...]

    def forward(g):
        @pl.when(q3 & lower & relayed(g))
        def _():
            x_side(g).wait_recv()
            via_down(g).start()

    def relay(g):
        @pl.when(has2)
        def _():
            x_two(g).wait_recv()
            x_relay(g).start()

    def compute(g):
        @pl.when(hasa)
        def _():
            x_chip(g).wait_recv()

        pl.when(has2)(lambda: x_relay(g).wait_recv())
        load_k(g).wait()
        load_v(g).wait()
        allowed = lax.broadcasted_iota(jnp.int32, (kbr, STEPS * qb), 0) <= offrow[...]
        for h in range(hc):
            c = slice(h * dh, (h + 1) * dh)
            qh = x[g, 0, :, c]
            doh = x[g, 1, :, c]
            kh = kb[g, :, c]
            vh = vb[g, :, c]
            row = pl.ds(g * hc + h, 1)
            s = dot(kh, qh, 1, 1) * scale - lse[row, :]
            p = jnp.where(allowed, jnp.exp(s), 0.0)
            dp = dot(vh, doh, 1, 1)
            ds = (p * (dp - dlt[row, :]) * scale).astype(BF16)
            out = pl.ds(pl.multiple_of(g * w + h * dh, dh), dh)
            vgb[:, out] = dot(p.astype(BF16), doh, 1, 0).astype(BF16)
            kgb[:, out] = dot(ds, qh, 1, 0).astype(BF16)
            dq = dot(ds, kh, 0, 0)
            own[g, :, c] = dq
            part[g, :, c] = dq.astype(BF16)
        pl.when(has2)(lambda: p_partner(g).start())
        for d in range(hn):
            pl.when(hasa)(lambda d=d: p_ahead(g, d).start())
            if d:
                p_own(g, d).start()

    def combine(g):
        @pl.when(has2)
        def _():
            p_partner(g).wait_recv()
            both = own[g, 2 * qb:3 * qb, :] + got[g].astype(F32)
            part[g, 2 * qb:3 * qb, :] = both.astype(BF16)
            for d in range(hn):
                p_two(g, d).start()

    def finish(g):
        for d in range(hn):
            hs = lax.rem(hd + d, hn)
            if d:
                arrived(0, g, hs).wait()
                total = mate[0, hs, g].astype(F32)
            else:
                total = own[g, pl.ds(piece(hd), rows_out), :]
            here = pl.ds(pl.multiple_of(hs * feats + g * w, w), w)

            @pl.when(toc)
            def _():
                arrived(1, g, hs).wait()

            @pl.when(to2)
            def _():
                arrived(2, g, hs).wait()

            total = total + jnp.where(toc, mate[1, hs, g].astype(F32), 0.0)
            total = total + jnp.where(to2, mate[2, hs, g].astype(F32), 0.0)
            outb[:, here] = total.astype(BF16)

    for g in range(min(AHEAD, chunks)):
        forward(g)
    relay(0)

    for o in range(1, STEPS):
        pl.when(me + o < n)(lambda o=o: st_send(o).wait_recv())
    for o in range(STEPS):
        lse[:, o * qb:(o + 1) * qb] = st[o, :, 0:qb]
        dlt[:, o * qb:(o + 1) * qb] = st[o, :, qb:2 * qb]

    def sent(t):
        below = jnp.clip((t - WAIT0) * RATE0, 0, t - LAG0)
        return jnp.clip(jnp.where((quad < 2) & (me + 4 < n), below, t - LAG1), 0, chunks)

    @pl.loop(1, chunks + 1)
    def _(t):
        pl.when(t + AHEAD - 1 < chunks)(lambda: forward(t + AHEAD - 1))
        pl.when(t < chunks)(lambda: relay(t))
        compute(t - 1)

        @pl.loop(sent(t - 1), sent(t))
        def _(g):
            combine(g)

    @pl.loop(sent(chunks), chunks)
    def _(g):
        combine(g)

    @pl.loop(0, chunks)
    def _(g):
        pl.when(q2 | q3 | lower)(lambda: x_two(g).wait_send())
        pl.when(odd | lower)(lambda: x_chip(g).wait_send())
        pl.when(q3 & lower & relayed(g))(lambda: via_down(g).wait_send())

        @pl.when(has2)
        def _():
            x_relay(g).wait_send()
            p_partner(g).wait_send()

        for d in range(1, hn):
            p_own(g, d).wait_send()

    for o in range(1, STEPS):
        pl.when(me >= o)(lambda o=o: st_send(o).wait_send())

    @pl.loop(0, chunks)
    def _(g):
        finish(g)
        for d in range(hn):
            pl.when(hasa)(lambda d=d: p_ahead(g, d).wait_send())
            pl.when(has2)(lambda d=d: p_two(g, d).wait_send())


def write_out(kgb, vgb, outb, kg_hbm, vg_hbm, qg_hbm, sem):
    copies = [
        pltpu.make_async_copy(src, dst, sem.at[i])
        for i, (src, dst) in enumerate(((kgb, kg_hbm), (vgb, vg_hbm), (outb, qg_hbm)))
    ]
    for copy in copies:
        copy.start()
    for copy in copies:
        copy.wait()


def per_device(query, query_offset, attn_out, out_grad, log_norm, keys, values):
    n = lax.axis_size("seq")
    hn = lax.axis_size("head")
    heads = log_norm.shape[0]
    qb, feats = query.shape
    kbr = keys.shape[0]
    dh = feats // heads
    hc = HEADS_PER_CHUNK
    while heads % hc:
        hc -= 1
    chunks = heads // hc
    w = hc * dh
    dims = (n, hn, heads, hc, dh, qb, kbr)
    span = STEPS * qb
    dma = pltpu.SemaphoreType.DMA
    args = (query, query_offset.reshape(1, qb), attn_out, out_grad, log_norm, keys, values)
    outs = (
        jax.ShapeDtypeStruct((kbr, feats), BF16),
        jax.ShapeDtypeStruct((kbr, feats), BF16),
        jax.ShapeDtypeStruct((qb // hn, feats * hn), BF16),
    )
    grads = pl.pallas_call(
        functools.partial(kernel, dims),
        out_shape=tuple(pltpu.VMEM(o.shape, o.dtype) for o in outs),
        in_specs=[pl.BlockSpec(memory_space=pl.ANY)] * 7,
        out_specs=tuple([pl.BlockSpec(memory_space=pltpu.VMEM)] * 3),
        scratch_shapes=[
            pltpu.VMEM((chunks, 2, span, w), BF16),
            pltpu.VMEM((chunks, 2, qb, w), BF16),
            pltpu.VMEM((chunks, kbr, w), BF16),
            pltpu.VMEM((chunks, kbr, w), BF16),
            pltpu.VMEM((qb, feats), BF16),
            pltpu.VMEM((heads, qb), F32),
            pltpu.VMEM((1, qb), jnp.int32),
            pltpu.VMEM((STEPS, heads, 2 * qb), F32),
            pltpu.VMEM((heads, span), F32),
            pltpu.VMEM((heads, span), F32),
            pltpu.VMEM((1, span), jnp.int32),
            pltpu.VMEM((chunks, span, w), F32),
            pltpu.VMEM((chunks, span, w), BF16),
            pltpu.VMEM((chunks, qb, w), BF16),
            pltpu.VMEM((3, hn, chunks, qb // hn, w), BF16),
            dma((2, chunks)), dma((2, chunks)), dma((3,)),
            dma((4, chunks)), dma((4, chunks)), dma((3,)), dma((3,)),
            dma((chunks,)), dma((chunks,)),
            dma((3, hn, chunks)), dma((3, hn, chunks)),
        ],
        compiler_params=pltpu.CompilerParams(
            collective_id=0, has_side_effects=True, vmem_limit_bytes=40 * 1024 * 1024
        ),
    )(*[pltpu.with_memory_space_constraint(a, pltpu.HBM) for a in args])
    return pl.pallas_call(
        write_out,
        out_shape=outs,
        in_specs=[pl.BlockSpec(memory_space=pltpu.VMEM)] * 3,
        out_specs=tuple([pl.BlockSpec(memory_space=pl.ANY)] * 3),
        scratch_shapes=[dma((3,))],
        compiler_params=pltpu.CompilerParams(vmem_limit_bytes=16 * 1024 * 1024),
    )(*grads)


def solution(mesh):
    in_specs = (
        P("seq", "head"),
        P("seq"),
        P("seq", "head"),
        P("seq", "head"),
        P("head", "seq"),
        P("seq", "head"),
        P("seq", "head"),
    )
    out_specs = (P("seq", "head"), P("seq", "head"), P(("seq", "head"), None))
    return jax.shard_map(
        per_device, mesh=mesh, in_specs=in_specs, out_specs=out_specs, check_vma=False
    )
```

```python
import functools
import math

import jax
import jax.numpy as jnp
from jax import lax
from jax.experimental import pallas as pl
from jax.experimental.pallas import tpu as pltpu
from jax.sharding import PartitionSpec as P

STEPS = 4
HEADS_PER_CHUNK = 2
LAG0 = 1
LAG1 = 1
WAIT1 = 0
RATE1 = 9
WAIT0 = 5
RATE0 = 2
FROM = 2
UPTO = 8
AHEAD = 3
F32 = jnp.float32
BF16 = jnp.bfloat16


def dot(a, b, ca, cb):
    return lax.dot_general(a, b, (((ca,), (cb,)), ((), ())), preferred_element_type=F32)


def kernel(
    dims, q_hbm, off_hbm, o_hbm, do_hbm, ln_hbm, k_hbm, v_hbm,
    kgb, vgb, outb,
    x, via, kb, vb, ob, lnb, offb, st, lse, dlt, offrow, own, part, got, mate,
    small_sem, xs, xr, ss, sr, ps, pr, rsnd, rrcv, ready,
):
    n, hn, heads, hc, dh, qb, kbr = dims
    chunks = heads // hc
    w = hc * dh
    feats = heads * dh
    rows_out = qb // hn
    scale = 1.0 / math.sqrt(dh)
    me = lax.axis_index("seq")
    hd = lax.axis_index("head")
    k = lax.rem(me, 2)
    partner = me + 1 - 2 * k
    oa = 1 + 2 * k
    oc = 3 - 2 * k
    quad = lax.rem(me, 4)
    q0, q1, q2, q3 = (quad == i for i in range(4))
    odd = k == 1
    lower = me >= 4
    has2 = me + 2 < n
    hasa = me + oa < n
    to2 = me >= 2
    toc = me >= oc

    def drain(ref, sem):
        pltpu.make_async_copy(ref, ref, sem).wait()

    def rows(o):
        return pl.ds(pl.multiple_of(o * qb, qb), qb)

    def cols(g):
        return pl.ds(pl.multiple_of(g * w, w), w)

    def load_q(g):
        return pltpu.make_async_copy(q_hbm.at[:, cols(g)], x.at[g, 0, pl.ds(0, qb)], small_sem.at[3])

    def load_do(g):
        return pltpu.make_async_copy(do_hbm.at[:, cols(g)], x.at[g, 1, pl.ds(0, qb)], small_sem.at[3])

    load_k = pltpu.make_async_copy(k_hbm, kb, small_sem.at[4])
    load_v = pltpu.make_async_copy(v_hbm, vb, small_sem.at[5])
    load_o = pltpu.make_async_copy(o_hbm, ob, small_sem.at[0])
    load_ln = pltpu.make_async_copy(ln_hbm, lnb, small_sem.at[1])
    load_off = pltpu.make_async_copy(off_hbm, offb, small_sem.at[2])

    def remote(src, dst, send, recv, target):
        return pltpu.make_async_remote_copy(
            src_ref=src, dst_ref=dst, send_sem=send, recv_sem=recv,
            device_id={"seq": target}, device_id_type=pl.DeviceIdType.MESH,
        )

    def mine(g):
        return x.at[g, :, pl.ds(0, qb)]

    def slot(g, o):
        return x.at[g, :, rows(o)]

    def x_two(g):
        return remote(mine(g), slot(g, 2), xs.at[0], xr.at[0, g], me - 2)

    def x_chip(g):
        return remote(mine(g), slot(g, 1), xs.at[1], xr.at[1, g], me - 1)

    def x_three(g):
        return remote(mine(g), slot(g, 3), xs.at[1], xr.at[1, g], me - 3)

    def x_side(g):
        return remote(mine(g), via.at[g], xs.at[0], xr.at[3, g], me + 3)

    def via_down(g):
        return remote(via.at[g], slot(g, 2), xs.at[3], xr.at[0, g], me - 5)

    start = chunks * FROM // 10
    upto = chunks * UPTO // 10

    def relayed(g):
        return (g >= start) & (g < upto)

    def x_relay(g):
        return remote(slot(g, 2), slot(g, oa), xs.at[2], xr.at[2, g], partner)

    def st_send(o):
        return remote(st.at[0], st.at[o], ss.at[o - 1], sr.at[o - 1], me - o)

    def p_partner(g):
        return remote(part.at[g, rows(oc)], got.at[g], ps, pr.at[g], partner)

    def piece(hs):
        return pl.multiple_of(hs * rows_out, rows_out)

    def back(kind, g, d, ahead, o):
        peer = lax.rem(hd + d, hn)
        return pltpu.make_async_remote_copy(
            src_ref=part.at[g, pl.ds(pl.multiple_of(o * qb, qb) + piece(peer), rows_out)],
            dst_ref=mate.at[kind, hd, g], send_sem=rsnd.at[kind, d], recv_sem=rrcv.at[order(kind, g), hd],
            device_id={"seq": me + ahead, "head": peer}, device_id_type=pl.DeviceIdType.MESH,
        )

    def p_own(g, d):
        return back(0, g, d, 0, 0)

    def p_ahead(g, d):
        return back(1, g, d, oa, oa)

    def p_two(g, d):
        return back(2, g, d, 2, 2)

    bulk = max(chunks - 2, 0)

    def order(kind, g):
        return kind + jnp.maximum(g - bulk + 1, 0) if kind == 2 else kind

    barrier = pltpu.get_barrier_semaphore()

    def greet(cond, ahead, d=0):
        @pl.when(cond)
        def _():
            pl.semaphore_signal(
                barrier, inc=1, device_id={"seq": me + ahead, "head": lax.rem(hd + d, hn)},
                device_id_type=pl.DeviceIdType.MESH,
            )

        return cond.astype(jnp.int32)

    peers = 0
    for o in range(1, STEPS):
        peers = peers + greet(me >= o, -o) + greet(me + o < n, o)
    peers = peers + greet(q3 & lower, -5) + greet(q2 & (me + 5 < n), 5)
    for d in range(1, hn):
        peers = peers + greet(me >= 0, 0, d)

    @pl.loop(0, chunks)
    def _(g):
        load_do(g).start()
        load_q(g).start()

    load_o.start()
    load_ln.start()
    load_off.start()

    load_o.wait()
    load_ln.wait()

    drain(x.at[:, :, pl.ds(0, qb)], small_sem.at[3])

    st[0, :, 0:qb] = lnb[...]
    eye = lax.broadcasted_iota(jnp.int32, (qb, qb), 0) == lax.broadcasted_iota(jnp.int32, (qb, qb), 1)
    for h in range(heads):
        oh = ob[:, h * dh:(h + 1) * dh]
        doh = x[h // hc, 1, 0:qb, h % hc * dh:(h % hc + 1) * dh]
        t = dot(oh, doh, 1, 1)
        st[0, h:h + 1, qb:2 * qb] = jnp.sum(jnp.where(eye, t, 0.0), axis=0, keepdims=True)

    pl.semaphore_wait(barrier, peers)
    for d in range(1, hn):
        pl.semaphore_signal(
            ready, inc=1, device_id={"head": lax.rem(hd + d, hn)}, device_id_type=pl.DeviceIdType.MESH
        )

    def send_x(g):
        pl.when(q2 | q3 | (lower & (q1 | (q0 & jnp.logical_not(relayed(g))))))(lambda: x_two(g).start())
        pl.when(q0 & lower & relayed(g))(lambda: x_side(g).start())
        pl.when(odd)(lambda: x_chip(g).start())
        pl.when((q0 | q2) & lower)(lambda: x_three(g).start())

    for o in range(1, STEPS):
        pl.when(me >= o)(lambda o=o: st_send(o).start())

    @pl.loop(0, chunks)
    def _(g):
        send_x(g)

    load_k.start()
    load_v.start()

    for o in range(1, STEPS):

        @pl.when(me + o >= n)
        def _(o=o):
            @pl.loop(0, chunks)
            def _(g):
                for i in range(2):
                    x[g, i, rows(o), :] = jnp.zeros((qb, w), BF16)

            st[o] = jnp.zeros_like(st[o])

    load_off.wait()
    offrow[...] = jnp.full(offrow.shape, kbr, jnp.int32)
    offrow[:, 0:qb] = offb[...]

    def forward(g):
        @pl.when(q3 & lower & relayed(g))
        def _():
            x_side(g).wait_recv()
            via_down(g).start()

    def relay(g):
        @pl.when(has2)
        def _():
            x_two(g).wait_recv()
            x_relay(g).start()

    def compute(g):
        @pl.when(hasa)
        def _():
            x_chip(g).wait_recv()

        pl.when(has2)(lambda: x_relay(g).wait_recv())
        allowed = lax.broadcasted_iota(jnp.int32, (kbr, STEPS * qb), 0) <= offrow[...]
        for h in range(hc):
            c = slice(h * dh, (h + 1) * dh)
            qh = x[g, 0, :, c]
            doh = x[g, 1, :, c]
            out = pl.ds(pl.multiple_of(g * w + h * dh, dh), dh)
            kh = kb[:, out]
            vh = vb[:, out]
            row = pl.ds(g * hc + h, 1)
            s = dot(kh, qh, 1, 1) * scale - lse[row, :]
            p = jnp.where(allowed, jnp.exp(s), 0.0)
            dp = dot(vh, doh, 1, 1)
            ds = (p * (dp - dlt[row, :]) * scale).astype(BF16)
            vgb[:, out] = dot(p.astype(BF16), doh, 1, 0).astype(BF16)
            kgb[:, out] = dot(ds, qh, 1, 0).astype(BF16)
            dq = dot(ds, kh, 0, 0)
            own[g, :, c] = dq
            part[g, :, c] = dq.astype(BF16)
        pl.when(has2)(lambda: p_partner(g).start())
        for d in range(hn):
            pl.when(hasa)(lambda d=d: p_ahead(g, d).start())
            if d:
                p_own(g, d).start()

    def combine(g):
        @pl.when(has2)
        def _():
            p_partner(g).wait_recv()
            both = own[g, 2 * qb:3 * qb, :] + got[g].astype(F32)
            part[g, 2 * qb:3 * qb, :] = both.astype(BF16)
            for d in range(hn):
                p_two(g, d).start()

    def finish(g):
        for d in range(hn):
            hs = lax.rem(hd + d, hn)
            total = mate[0, hs, g].astype(F32) if d else own[g, pl.ds(piece(hd), rows_out), :]
            total = total + jnp.where(toc, mate[1, hs, g].astype(F32), 0.0)
            total = total + jnp.where(to2, mate[2, hs, g].astype(F32), 0.0)
            outb[:, pl.ds(pl.multiple_of(hs * feats + g * w, w), w)] = total.astype(BF16)

    for g in range(min(AHEAD, chunks)):
        forward(g)
    relay(0)

    for o in range(1, STEPS):
        pl.when(me + o < n)(lambda o=o: st_send(o).wait_recv())
    for o in range(STEPS):
        lse[:, o * qb:(o + 1) * qb] = st[o, :, 0:qb]
        dlt[:, o * qb:(o + 1) * qb] = st[o, :, qb:2 * qb]

    def sent(t):
        low = jnp.where(me + 4 < n, jnp.clip((t - WAIT0) * RATE0, 0, t - LAG0), t - LAG0)
        high = jnp.clip((t - WAIT1) * RATE1, 0, t - LAG1)
        return jnp.clip(jnp.where(quad < 2, low, high), 0, chunks)

    pl.semaphore_wait(ready, hn - 1)
    load_k.wait()
    load_v.wait()

    @pl.loop(1, chunks + 1)
    def _(t):
        pl.when(t + AHEAD - 1 < chunks)(lambda: forward(t + AHEAD - 1))
        pl.when(t < chunks)(lambda: relay(t))
        compute(t - 1)

        @pl.loop(sent(t - 1), sent(t))
        def _(g):
            combine(g)

    @pl.loop(sent(chunks), chunks)
    def _(g):
        combine(g)

    sent_x = x.at[:, :, pl.ds(0, qb)]
    pl.when(q2 | q3 | lower)(lambda: drain(sent_x, xs.at[0]))
    pl.when(odd | lower)(lambda: drain(sent_x, xs.at[1]))
    pl.when(has2)(lambda: drain(x.at[:, :, rows(2)], xs.at[2]))
    if upto > start:
        pl.when(q3 & lower)(lambda: drain(via.at[pl.ds(start, upto - start)], xs.at[3]))
    pl.when(has2)(lambda: drain(part.at[:, rows(oc)], ps))
    for o in range(1, STEPS):
        pl.when(me >= o)(lambda o=o: st_send(o).wait_send())

    for d in range(hn):
        hs = lax.rem(hd + d, hn)
        if d:
            drain(part.at[:, pl.ds(0, rows_out)], rsnd.at[0, d])
            drain(mate.at[0, hs], rrcv.at[0, hs])
        pl.when(hasa)(lambda d=d: drain(part.at[:, pl.ds(0, rows_out)], rsnd.at[1, d]))
        pl.when(toc)(lambda hs=hs: drain(mate.at[1, hs], rrcv.at[1, hs]))
        if bulk:
            pl.when(to2)(lambda hs=hs: drain(mate.at[2, hs, pl.ds(0, bulk)], rrcv.at[2, hs]))

    @pl.loop(0, bulk)
    def _(g):
        finish(g)

    for g in range(bulk, chunks):
        for hs in range(hn):
            pl.when(to2)(lambda g=g, hs=hs: drain(mate.at[2, hs, g], rrcv.at[order(2, g), hs]))
        finish(g)

    for d in range(hn):
        pl.when(has2)(lambda d=d: drain(part.at[:, pl.ds(0, rows_out)], rsnd.at[2, d]))


def write_out(kgb, vgb, outb, kg_hbm, vg_hbm, qg_hbm, sem):
    copies = [
        pltpu.make_async_copy(src, dst, sem.at[i])
        for i, (src, dst) in enumerate(((kgb, kg_hbm), (vgb, vg_hbm), (outb, qg_hbm)))
    ]
    for copy in copies:
        copy.start()
    for copy in copies:
        copy.wait()


def per_device(query, query_offset, attn_out, out_grad, log_norm, keys, values):
    n = lax.axis_size("seq")
    hn = lax.axis_size("head")
    heads = log_norm.shape[0]
    qb, feats = query.shape
    kbr = keys.shape[0]
    dh = feats // heads
    hc = HEADS_PER_CHUNK
    while heads % hc:
        hc -= 1
    chunks = heads // hc
    w = hc * dh
    dims = (n, hn, heads, hc, dh, qb, kbr)
    span = STEPS * qb
    dma = pltpu.SemaphoreType.DMA
    args = (query, query_offset.reshape(1, qb), attn_out, out_grad, log_norm, keys, values)
    outs = (
        jax.ShapeDtypeStruct((kbr, feats), BF16),
        jax.ShapeDtypeStruct((kbr, feats), BF16),
        jax.ShapeDtypeStruct((qb // hn, feats * hn), BF16),
    )
    grads = pl.pallas_call(
        functools.partial(kernel, dims),
        out_shape=tuple(pltpu.VMEM(o.shape, o.dtype) for o in outs),
        in_specs=[pl.BlockSpec(memory_space=pl.ANY)] * 7,
        out_specs=tuple([pl.BlockSpec(memory_space=pltpu.VMEM)] * 3),
        scratch_shapes=[
            pltpu.VMEM((chunks, 2, span, w), BF16),
            pltpu.VMEM((chunks, 2, qb, w), BF16),
            pltpu.VMEM((kbr, feats), BF16),
            pltpu.VMEM((kbr, feats), BF16),
            pltpu.VMEM((qb, feats), BF16),
            pltpu.VMEM((heads, qb), F32),
            pltpu.VMEM((1, qb), jnp.int32),
            pltpu.VMEM((STEPS, heads, 2 * qb), F32),
            pltpu.VMEM((heads, span), F32),
            pltpu.VMEM((heads, span), F32),
            pltpu.VMEM((1, span), jnp.int32),
            pltpu.VMEM((chunks, span, w), F32),
            pltpu.VMEM((chunks, span, w), BF16),
            pltpu.VMEM((chunks, qb, w), BF16),
            pltpu.VMEM((3, hn, chunks, qb // hn, w), BF16),
            dma((6,)), dma((4,)), dma((4, chunks)), dma((3,)), dma((3,)),
            dma(()), dma((chunks,)), dma((3, hn)), dma((5, hn)), pltpu.SemaphoreType.REGULAR,
        ],
        compiler_params=pltpu.CompilerParams(
            collective_id=0, has_side_effects=True, vmem_limit_bytes=40 * 1024 * 1024
        ),
    )(*[pltpu.with_memory_space_constraint(a, pltpu.HBM) for a in args])
    return pl.pallas_call(
        write_out,
        out_shape=outs,
        in_specs=[pl.BlockSpec(memory_space=pltpu.VMEM)] * 3,
        out_specs=tuple([pl.BlockSpec(memory_space=pl.ANY)] * 3),
        scratch_shapes=[dma((3,))],
        compiler_params=pltpu.CompilerParams(vmem_limit_bytes=16 * 1024 * 1024),
    )(*grads)


def solution(mesh):
    in_specs = (
        P("seq", "head"),
        P("seq"),
        P("seq", "head"),
        P("seq", "head"),
        P("head", "seq"),
        P("seq", "head"),
        P("seq", "head"),
    )
    out_specs = (P("seq", "head"), P("seq", "head"), P(("seq", "head"), None))
    return jax.shard_map(
        per_device, mesh=mesh, in_specs=in_specs, out_specs=out_specs, check_vma=False
    )
```

```python
import functools
import math

import jax
import jax.numpy as jnp
from jax import lax
from jax.experimental import pallas as pl
from jax.experimental.pallas import tpu as pltpu
from jax.sharding import PartitionSpec as P

STEPS = 4
HEADS_PER_CHUNK = 2
LAG0 = 1
LAG1 = 1
WAIT1 = 2
RATE1 = 3
WAIT0 = 6
RATE0 = 3
FROM = 2
UPTO = 8
AHEAD = 3
F32 = jnp.float32
BF16 = jnp.bfloat16


def dot(a, b, ca, cb):
    return lax.dot_general(a, b, (((ca,), (cb,)), ((), ())), preferred_element_type=F32)


def kernel(
    dims, q_hbm, off_hbm, o_hbm, do_hbm, ln_hbm, k_hbm, v_hbm,
    kgb, vgb, outb,
    x, via, kb, vb, ob, lnb, offb, st, lse, dlt, offrow, own, part, got, mate, pb, db,
    small_sem, xs, xr, ss, sr, ps, pr, rsnd, rrcv, ready,
):
    n, hn, heads, hc, dh, qb, kbr = dims
    chunks = heads // hc
    w = hc * dh
    feats = heads * dh
    rows_out = qb // hn
    scale = 1.0 / math.sqrt(dh)
    me = lax.axis_index("seq")
    hd = lax.axis_index("head")
    k = lax.rem(me, 2)
    partner = me + 1 - 2 * k
    oa = 1 + 2 * k
    oc = 3 - 2 * k
    quad = lax.rem(me, 4)
    q0, q1, q2, q3 = (quad == i for i in range(4))
    odd = k == 1
    lower = me >= 4
    has2 = me + 2 < n
    hasa = me + oa < n
    to2 = me >= 2
    toc = me >= oc

    def drain(ref, sem):
        pltpu.make_async_copy(ref, ref, sem).wait()

    def rows(o):
        return pl.ds(pl.multiple_of(o * qb, qb), qb)

    def cols(g):
        return pl.ds(pl.multiple_of(g * w, w), w)

    def load_q(g):
        return pltpu.make_async_copy(q_hbm.at[:, cols(g)], x.at[g, 0, pl.ds(0, qb)], small_sem.at[3])

    def load_do(g):
        return pltpu.make_async_copy(do_hbm.at[:, cols(g)], x.at[g, 1, pl.ds(0, qb)], small_sem.at[3])

    load_k = pltpu.make_async_copy(k_hbm, kb, small_sem.at[4])
    load_v = pltpu.make_async_copy(v_hbm, vb, small_sem.at[5])
    load_o = pltpu.make_async_copy(o_hbm, ob, small_sem.at[0])
    load_ln = pltpu.make_async_copy(ln_hbm, lnb, small_sem.at[1])
    load_off = pltpu.make_async_copy(off_hbm, offb, small_sem.at[2])

    def remote(src, dst, send, recv, target):
        return pltpu.make_async_remote_copy(
            src_ref=src, dst_ref=dst, send_sem=send, recv_sem=recv,
            device_id={"seq": target}, device_id_type=pl.DeviceIdType.MESH,
        )

    def mine(g):
        return x.at[g, :, pl.ds(0, qb)]

    def slot(g, o):
        return x.at[g, :, rows(o)]

    def x_two(g):
        return remote(mine(g), slot(g, 2), xs.at[0], xr.at[0, g], me - 2)

    def x_chip(g):
        return remote(mine(g), slot(g, 1), xs.at[1], xr.at[1, g], me - 1)

    def x_three(g):
        return remote(mine(g), slot(g, 3), xs.at[1], xr.at[1, g], me - 3)

    def x_side(g):
        return remote(mine(g), via.at[g], xs.at[0], xr.at[3, g], me + 3)

    def via_down(g):
        return remote(via.at[g], slot(g, 2), xs.at[3], xr.at[0, g], me - 5)

    start = chunks * FROM // 10
    upto = chunks * UPTO // 10

    def relayed(g):
        return (g >= start) & (g < upto)

    def x_relay(g):
        return remote(slot(g, 2), slot(g, oa), xs.at[2], xr.at[2, g], partner)

    def st_send(o):
        return remote(st.at[0], st.at[o], ss.at[o - 1], sr.at[o - 1], me - o)

    def p_partner(g):
        return remote(part.at[g, rows(oc)], got.at[g], ps, pr.at[g], partner)

    def piece(hs):
        return pl.multiple_of(hs * rows_out, rows_out)

    def back(kind, g, d, ahead, o):
        peer = lax.rem(hd + d, hn)
        return pltpu.make_async_remote_copy(
            src_ref=part.at[g, pl.ds(pl.multiple_of(o * qb, qb) + piece(peer), rows_out)],
            dst_ref=mate.at[kind, hd, g], send_sem=rsnd.at[kind, d], recv_sem=rrcv.at[order(kind, g), hd],
            device_id={"seq": me + ahead, "head": peer}, device_id_type=pl.DeviceIdType.MESH,
        )

    def p_own(g, d):
        return back(0, g, d, 0, 0)

    def p_ahead(g, d):
        return back(1, g, d, oa, oa)

    def p_two(g, d):
        return back(2, g, d, 2, 2)

    bulk = max(chunks - 2, 0)

    def order(kind, g):
        return kind + jnp.maximum(g - bulk + 1, 0) if kind == 2 else kind

    barrier = pltpu.get_barrier_semaphore()

    def greet(cond, ahead, d=0):
        @pl.when(cond)
        def _():
            pl.semaphore_signal(
                barrier, inc=1, device_id={"seq": me + ahead, "head": lax.rem(hd + d, hn)},
                device_id_type=pl.DeviceIdType.MESH,
            )

        return cond.astype(jnp.int32)

    peers = 0
    for o in range(1, STEPS):
        peers = peers + greet(me >= o, -o) + greet(me + o < n, o)
    peers = peers + greet(q3 & lower, -5) + greet(q2 & (me + 5 < n), 5)
    for d in range(1, hn):
        peers = peers + greet(me >= 0, 0, d)

    @pl.loop(0, chunks)
    def _(g):
        load_do(g).start()
        load_q(g).start()

    load_o.start()
    load_ln.start()
    load_off.start()

    drain(x.at[:, :, pl.ds(0, qb)], small_sem.at[3])

    pl.semaphore_wait(barrier, peers)
    for d in range(1, hn):
        pl.semaphore_signal(
            ready, inc=1, device_id={"head": lax.rem(hd + d, hn)}, device_id_type=pl.DeviceIdType.MESH
        )

    def send_x(g):
        pl.when(q2 | q3 | (lower & (q1 | (q0 & jnp.logical_not(relayed(g))))))(lambda: x_two(g).start())
        pl.when(q0 & lower & relayed(g))(lambda: x_side(g).start())
        pl.when(odd)(lambda: x_chip(g).start())
        pl.when((q0 | q2) & lower)(lambda: x_three(g).start())

    send_x(0)

    load_o.wait()
    load_ln.wait()

    st[0, :, 0:qb] = lnb[...]
    eye = lax.broadcasted_iota(jnp.int32, (qb, qb), 0) == lax.broadcasted_iota(jnp.int32, (qb, qb), 1)
    for h in range(heads):
        oh = ob[:, h * dh:(h + 1) * dh]
        doh = x[h // hc, 1, 0:qb, h % hc * dh:(h % hc + 1) * dh]
        t = dot(oh, doh, 1, 1)
        st[0, h:h + 1, qb:2 * qb] = jnp.sum(jnp.where(eye, t, 0.0), axis=0, keepdims=True)

    for o in range(1, STEPS):
        pl.when(me >= o)(lambda o=o: st_send(o).start())

    @pl.loop(1, chunks)
    def _(g):
        send_x(g)

    load_k.start()
    load_v.start()

    for o in range(1, STEPS):

        @pl.when(me + o >= n)
        def _(o=o):
            @pl.loop(0, chunks)
            def _(g):
                for i in range(2):
                    x[g, i, rows(o), :] = jnp.zeros((qb, w), BF16)

            st[o] = jnp.zeros_like(st[o])

    load_off.wait()
    offrow[...] = jnp.full(offrow.shape, kbr, jnp.int32)
    offrow[:, 0:qb] = offb[...]

    def forward(g):
        @pl.when(q3 & lower & relayed(g))
        def _():
            x_side(g).wait_recv()
            via_down(g).start()

    def relay(g):
        @pl.when(has2)
        def _():
            x_two(g).wait_recv()
            x_relay(g).start()

    def compute(g):
        @pl.when(hasa)
        def _():
            x_chip(g).wait_recv()

        pl.when(has2)(lambda: x_relay(g).wait_recv())
        half = 2 * qb
        allowed = lax.broadcasted_iota(jnp.int32, (kbr, half), 0) <= offrow[:, 0:half]
        for h in range(hc):
            c = slice(h * dh, (h + 1) * dh)
            out = pl.ds(pl.multiple_of(g * w + h * dh, dh), dh)
            row = pl.ds(g * hc + h, 1)
            s = dot(kb[:, out], x[g, 0, :, c], 1, 1) * scale - lse[row, :]
            p = jnp.exp(s)
            p = jnp.concatenate([jnp.where(allowed, p[:, 0:half], 0.0), p[:, half:]], axis=1)
            pb[h] = p.astype(BF16)
            dp = dot(vb[:, out], x[g, 1, :, c], 1, 1)
            db[h] = (p * (dp - dlt[row, :]) * scale).astype(BF16)
        for h in range(hc):
            c = slice(h * dh, (h + 1) * dh)
            out = pl.ds(pl.multiple_of(g * w + h * dh, dh), dh)
            vgb[:, out] = dot(pb[h], x[g, 1, :, c], 1, 0).astype(BF16)
            kgb[:, out] = dot(db[h], x[g, 0, :, c], 1, 0).astype(BF16)
            dq = dot(db[h], kb[:, out], 0, 0)
            own[g, :, c] = dq
            part[g, :, c] = dq.astype(BF16)
        pl.when(has2)(lambda: p_partner(g).start())
        for d in range(hn):
            pl.when(hasa)(lambda d=d: p_ahead(g, d).start())
            if d:
                p_own(g, d).start()

    def combine(g):
        @pl.when(has2)
        def _():
            p_partner(g).wait_recv()
            both = own[g, 2 * qb:3 * qb, :] + got[g].astype(F32)
            part[g, 2 * qb:3 * qb, :] = both.astype(BF16)
            for d in range(hn):
                p_two(g, d).start()

    def finish(g):
        for d in range(hn):
            hs = lax.rem(hd + d, hn)
            total = mate[0, hs, g].astype(F32) if d else own[g, pl.ds(piece(hd), rows_out), :]
            total = total + jnp.where(toc, mate[1, hs, g].astype(F32), 0.0)
            total = total + jnp.where(to2, mate[2, hs, g].astype(F32), 0.0)
            outb[:, pl.ds(pl.multiple_of(hs * feats + g * w, w), w)] = total.astype(BF16)

    for g in range(min(AHEAD, chunks)):
        forward(g)
    relay(0)

    for o in range(1, STEPS):
        pl.when(me + o < n)(lambda o=o: st_send(o).wait_recv())
    for o in range(STEPS):
        lse[:, o * qb:(o + 1) * qb] = st[o, :, 0:qb]
        dlt[:, o * qb:(o + 1) * qb] = st[o, :, qb:2 * qb]

    def sent(t):
        low = jnp.where(me + 4 < n, jnp.clip((t - WAIT0) * RATE0, 0, t - LAG0), t - LAG0)
        high = jnp.clip((t - WAIT1) * RATE1, 0, t - LAG1)
        return jnp.clip(jnp.where(quad < 2, low, high), 0, chunks)

    pl.semaphore_wait(ready, hn - 1)
    load_k.wait()
    load_v.wait()

    @pl.loop(1, chunks + 1)
    def _(t):
        pl.when(t + AHEAD - 1 < chunks)(lambda: forward(t + AHEAD - 1))
        pl.when(t < chunks)(lambda: relay(t))
        compute(t - 1)

        @pl.loop(sent(t - 1), sent(t))
        def _(g):
            combine(g)

    @pl.loop(sent(chunks), chunks)
    def _(g):
        combine(g)

    sent_x = x.at[:, :, pl.ds(0, qb)]
    pl.when(q2 | q3 | lower)(lambda: drain(sent_x, xs.at[0]))
    pl.when(odd | lower)(lambda: drain(sent_x, xs.at[1]))
    pl.when(has2)(lambda: drain(x.at[:, :, rows(2)], xs.at[2]))
    if upto > start:
        pl.when(q3 & lower)(lambda: drain(via.at[pl.ds(start, upto - start)], xs.at[3]))
    pl.when(has2)(lambda: drain(part.at[:, rows(oc)], ps))
    for o in range(1, STEPS):
        pl.when(me >= o)(lambda o=o: st_send(o).wait_send())

    for d in range(hn):
        hs = lax.rem(hd + d, hn)
        if d:
            drain(part.at[:, pl.ds(0, rows_out)], rsnd.at[0, d])
            drain(mate.at[0, hs], rrcv.at[0, hs])
        pl.when(hasa)(lambda d=d: drain(part.at[:, pl.ds(0, rows_out)], rsnd.at[1, d]))
        pl.when(toc)(lambda hs=hs: drain(mate.at[1, hs], rrcv.at[1, hs]))
        if bulk:
            pl.when(to2)(lambda hs=hs: drain(mate.at[2, hs, pl.ds(0, bulk)], rrcv.at[2, hs]))

    @pl.loop(0, bulk)
    def _(g):
        finish(g)

    for g in range(bulk, chunks):
        for hs in range(hn):
            pl.when(to2)(lambda g=g, hs=hs: drain(mate.at[2, hs, g], rrcv.at[order(2, g), hs]))
        finish(g)

    for d in range(hn):
        pl.when(has2)(lambda d=d: drain(part.at[:, pl.ds(0, rows_out)], rsnd.at[2, d]))


def write_out(kgb, vgb, outb, kg_hbm, vg_hbm, qg_hbm, sem):
    copies = [
        pltpu.make_async_copy(src, dst, sem.at[i])
        for i, (src, dst) in enumerate(((kgb, kg_hbm), (vgb, vg_hbm), (outb, qg_hbm)))
    ]
    for copy in copies:
        copy.start()
    for copy in copies:
        copy.wait()


def per_device(query, query_offset, attn_out, out_grad, log_norm, keys, values):
    n = lax.axis_size("seq")
    hn = lax.axis_size("head")
    heads = log_norm.shape[0]
    qb, feats = query.shape
    kbr = keys.shape[0]
    dh = feats // heads
    hc = HEADS_PER_CHUNK
    while heads % hc:
        hc -= 1
    chunks = heads // hc
    w = hc * dh
    dims = (n, hn, heads, hc, dh, qb, kbr)
    span = STEPS * qb
    dma = pltpu.SemaphoreType.DMA
    args = (query, query_offset.reshape(1, qb), attn_out, out_grad, log_norm, keys, values)
    outs = (
        jax.ShapeDtypeStruct((kbr, feats), BF16),
        jax.ShapeDtypeStruct((kbr, feats), BF16),
        jax.ShapeDtypeStruct((qb // hn, feats * hn), BF16),
    )
    grads = pl.pallas_call(
        functools.partial(kernel, dims),
        out_shape=tuple(pltpu.VMEM(o.shape, o.dtype) for o in outs),
        in_specs=[pl.BlockSpec(memory_space=pl.ANY)] * 7,
        out_specs=tuple([pl.BlockSpec(memory_space=pltpu.VMEM)] * 3),
        scratch_shapes=[
            pltpu.VMEM((chunks, 2, span, w), BF16),
            pltpu.VMEM((chunks, 2, qb, w), BF16),
            pltpu.VMEM((kbr, feats), BF16),
            pltpu.VMEM((kbr, feats), BF16),
            pltpu.VMEM((qb, feats), BF16),
            pltpu.VMEM((heads, qb), F32),
            pltpu.VMEM((1, qb), jnp.int32),
            pltpu.VMEM((STEPS, heads, 2 * qb), F32),
            pltpu.VMEM((heads, span), F32),
            pltpu.VMEM((heads, span), F32),
            pltpu.VMEM((1, span), jnp.int32),
            pltpu.VMEM((chunks, span, w), F32),
            pltpu.VMEM((chunks, span, w), BF16),
            pltpu.VMEM((chunks, qb, w), BF16),
            pltpu.VMEM((3, hn, chunks, qb // hn, w), BF16),
            pltpu.VMEM((hc, kbr, span), BF16),
            pltpu.VMEM((hc, kbr, span), BF16),
            dma((6,)), dma((4,)), dma((4, chunks)), dma((3,)), dma((3,)),
            dma(()), dma((chunks,)), dma((3, hn)), dma((5, hn)), pltpu.SemaphoreType.REGULAR,
        ],
        compiler_params=pltpu.CompilerParams(
            collective_id=0, has_side_effects=True, vmem_limit_bytes=40 * 1024 * 1024
        ),
    )(*[pltpu.with_memory_space_constraint(a, pltpu.HBM) for a in args])
    return pl.pallas_call(
        write_out,
        out_shape=outs,
        in_specs=[pl.BlockSpec(memory_space=pltpu.VMEM)] * 3,
        out_specs=tuple([pl.BlockSpec(memory_space=pl.ANY)] * 3),
        scratch_shapes=[dma((3,))],
        compiler_params=pltpu.CompilerParams(vmem_limit_bytes=16 * 1024 * 1024),
    )(*grads)


def solution(mesh):
    in_specs = (
        P("seq", "head"),
        P("seq"),
        P("seq", "head"),
        P("seq", "head"),
        P("head", "seq"),
        P("seq", "head"),
        P("seq", "head"),
    )
    out_specs = (P("seq", "head"), P("seq", "head"), P(("seq", "head"), None))
    return jax.shard_map(
        per_device, mesh=mesh, in_specs=in_specs, out_specs=out_specs, check_vma=False
    )
```

```python
import functools
import math

import jax
import jax.numpy as jnp
from jax import lax
from jax.experimental import pallas as pl
from jax.experimental.pallas import tpu as pltpu
from jax.sharding import PartitionSpec as P

STEPS = 4
HEADS_PER_CHUNK = 2
LAG0 = 1
LAG1 = 1
WAIT1 = 2
RATE1 = 3
WAIT0 = 6
RATE0 = 3
FROM = 2
UPTO = 8
AHEAD = 3
F32 = jnp.float32
BF16 = jnp.bfloat16


def dot(a, b, ca, cb):
    return lax.dot_general(a, b, (((ca,), (cb,)), ((), ())), preferred_element_type=F32)


def kernel(
    dims, q_hbm, off_hbm, o_hbm, do_hbm, ln_hbm, k_hbm, v_hbm,
    kgb, vgb, outb,
    x, via, kb, vb, ob, lnb, offb, st, lse, dlt, offrow, own, part, got, mate, pb, db,
    small_sem, xs, xr, ss, sr, ps, pr, rsnd, rrcv, ready,
):
    n, hn, heads, hc, dh, qb, kbr = dims
    chunks = heads // hc
    w = hc * dh
    feats = heads * dh
    rows_out = qb // hn
    scale = 1.0 / math.sqrt(dh)
    me = lax.axis_index("seq")
    hd = lax.axis_index("head")
    k = lax.rem(me, 2)
    partner = me + 1 - 2 * k
    oa = 1 + 2 * k
    oc = 3 - 2 * k
    quad = lax.rem(me, 4)
    q0, q1, q2, q3 = (quad == i for i in range(4))
    odd = k == 1
    lower = me >= 4
    has2 = me + 2 < n
    hasa = me + oa < n
    to2 = me >= 2
    toc = me >= oc

    def drain(ref, sem):
        pltpu.make_async_copy(ref, ref, sem).wait()

    def rows(o):
        return pl.ds(pl.multiple_of(o * qb, qb), qb)

    def cols(g):
        return pl.ds(pl.multiple_of(g * w, w), w)

    def load_q(g):
        return pltpu.make_async_copy(q_hbm.at[:, cols(g)], x.at[g, 0, pl.ds(0, qb)], small_sem.at[3])

    def load_do(g):
        return pltpu.make_async_copy(do_hbm.at[:, cols(g)], x.at[g, 1, pl.ds(0, qb)], small_sem.at[3])

    load_k = pltpu.make_async_copy(k_hbm, kb, small_sem.at[4])
    load_v = pltpu.make_async_copy(v_hbm, vb, small_sem.at[5])
    load_o = pltpu.make_async_copy(o_hbm, ob, small_sem.at[0])
    load_ln = pltpu.make_async_copy(ln_hbm, lnb, small_sem.at[1])
    load_off = pltpu.make_async_copy(off_hbm, offb, small_sem.at[2])

    def remote(src, dst, send, recv, target):
        return pltpu.make_async_remote_copy(
            src_ref=src, dst_ref=dst, send_sem=send, recv_sem=recv,
            device_id={"seq": target}, device_id_type=pl.DeviceIdType.MESH,
        )

    def mine(g):
        return x.at[g, :, pl.ds(0, qb)]

    def slot(g, o):
        return x.at[g, :, rows(o)]

    def x_two(g):
        return remote(mine(g), slot(g, 2), xs.at[0], xr.at[0, g], me - 2)

    def x_chip(g):
        return remote(mine(g), slot(g, 1), xs.at[1], xr.at[1, g], me - 1)

    def x_three(g):
        return remote(mine(g), slot(g, 3), xs.at[1], xr.at[1, g], me - 3)

    def x_side(g):
        return remote(mine(g), via.at[g], xs.at[0], xr.at[3, g], me + 3)

    def via_down(g):
        return remote(via.at[g], slot(g, 2), xs.at[3], xr.at[0, g], me - 5)

    start = chunks * FROM // 10
    upto = chunks * UPTO // 10

    def relayed(g):
        return (g >= start) & (g < upto)

    def x_relay(g):
        return remote(slot(g, 2), slot(g, oa), xs.at[2], xr.at[2, g], partner)

    st_two = remote(st.at[0], st.at[2], ss.at[0], sr.at[0], me - 2)
    st_near = remote(st.at[0], st.at[oc], ss.at[1], sr.at[1], me - oc)
    st_relay = remote(st.at[2], st.at[oa], ss.at[2], sr.at[2], partner)

    def p_partner(g):
        return remote(part.at[g, rows(oc)], got.at[g], ps, pr.at[g], partner)

    def piece(hs):
        return pl.multiple_of(hs * rows_out, rows_out)

    def back(kind, g, d, ahead, o):
        peer = lax.rem(hd + d, hn)
        return pltpu.make_async_remote_copy(
            src_ref=part.at[g, pl.ds(pl.multiple_of(o * qb, qb) + piece(peer), rows_out)],
            dst_ref=mate.at[kind, hd, g], send_sem=rsnd.at[kind, d], recv_sem=rrcv.at[order(kind, g), hd],
            device_id={"seq": me + ahead, "head": peer}, device_id_type=pl.DeviceIdType.MESH,
        )

    def p_own(g, d):
        return back(0, g, d, 0, 0)

    def p_ahead(g, d):
        return back(1, g, d, oa, oa)

    def p_two(g, d):
        return back(2, g, d, 2, 2)

    bulk = max(chunks - 2, 0)

    def order(kind, g):
        return kind + jnp.maximum(g - bulk + 1, 0) if kind == 2 else kind

    barrier = pltpu.get_barrier_semaphore()

    def greet(cond, ahead, d=0):
        @pl.when(cond)
        def _():
            pl.semaphore_signal(
                barrier, inc=1, device_id={"seq": me + ahead, "head": lax.rem(hd + d, hn)},
                device_id_type=pl.DeviceIdType.MESH,
            )

        return cond.astype(jnp.int32)

    peers = 0
    for o in range(1, STEPS):
        peers = peers + greet(me >= o, -o) + greet(me + o < n, o)
    peers = peers + greet(q3 & lower, -5) + greet(q2 & (me + 5 < n), 5)
    for d in range(1, hn):
        peers = peers + greet(me >= 0, 0, d)

    @pl.loop(0, chunks)
    def _(g):
        load_do(g).start()
        load_q(g).start()

    load_o.start()
    load_ln.start()
    load_off.start()

    drain(x.at[:, :, pl.ds(0, qb)], small_sem.at[3])

    pl.semaphore_wait(barrier, peers)
    for d in range(1, hn):
        pl.semaphore_signal(
            ready, inc=1, device_id={"head": lax.rem(hd + d, hn)}, device_id_type=pl.DeviceIdType.MESH
        )

    def send_x(g):
        pl.when(q2 | q3 | (lower & (q1 | (q0 & jnp.logical_not(relayed(g))))))(lambda: x_two(g).start())
        pl.when(q0 & lower & relayed(g))(lambda: x_side(g).start())
        pl.when(odd)(lambda: x_chip(g).start())
        pl.when((q0 | q2) & lower)(lambda: x_three(g).start())

    send_x(0)

    load_o.wait()
    load_ln.wait()

    st[0, :, 0:qb] = lnb[...]
    eye = lax.broadcasted_iota(jnp.int32, (qb, qb), 0) == lax.broadcasted_iota(jnp.int32, (qb, qb), 1)
    for h in range(heads):
        oh = ob[:, h * dh:(h + 1) * dh]
        doh = x[h // hc, 1, 0:qb, h % hc * dh:(h % hc + 1) * dh]
        t = dot(oh, doh, 1, 1)
        st[0, h:h + 1, qb:2 * qb] = jnp.sum(jnp.where(eye, t, 0.0), axis=0, keepdims=True)

    pl.when(to2)(lambda: st_two.start())
    pl.when(toc)(lambda: st_near.start())

    @pl.loop(1, chunks)
    def _(g):
        send_x(g)

    load_k.start()
    load_v.start()

    for o in range(1, STEPS):

        @pl.when(me + o >= n)
        def _(o=o):
            @pl.loop(0, chunks)
            def _(g):
                for i in range(2):
                    x[g, i, rows(o), :] = jnp.zeros((qb, w), BF16)

            st[o] = jnp.zeros_like(st[o])

    load_off.wait()
    offrow[...] = jnp.full(offrow.shape, kbr, jnp.int32)
    offrow[:, 0:qb] = offb[...]

    def forward(g):
        @pl.when(q3 & lower & relayed(g))
        def _():
            x_side(g).wait_recv()
            via_down(g).start()

    def relay(g):
        @pl.when(has2)
        def _():
            x_two(g).wait_recv()
            x_relay(g).start()

    def compute(g):
        @pl.when(hasa)
        def _():
            x_chip(g).wait_recv()

        pl.when(has2)(lambda: x_relay(g).wait_recv())
        half = 2 * qb
        allowed = lax.broadcasted_iota(jnp.int32, (kbr, half), 0) <= offrow[:, 0:half]
        for h in range(hc):
            c = slice(h * dh, (h + 1) * dh)
            out = pl.ds(pl.multiple_of(g * w + h * dh, dh), dh)
            row = pl.ds(g * hc + h, 1)
            s = dot(kb[:, out], x[g, 0, :, c], 1, 1) * scale - lse[row, :]
            p = jnp.exp(s)
            p = jnp.concatenate([jnp.where(allowed, p[:, 0:half], 0.0), p[:, half:]], axis=1)
            pb[h] = p.astype(BF16)
            dp = dot(vb[:, out], x[g, 1, :, c], 1, 1)
            db[h] = (p * (dp - dlt[row, :]) * scale).astype(BF16)
        for h in range(hc):
            c = slice(h * dh, (h + 1) * dh)
            out = pl.ds(pl.multiple_of(g * w + h * dh, dh), dh)
            vgb[:, out] = dot(pb[h], x[g, 1, :, c], 1, 0).astype(BF16)
            kgb[:, out] = dot(db[h], x[g, 0, :, c], 1, 0).astype(BF16)
            dq = dot(db[h], kb[:, out], 0, 0)
            own[g, :, c] = dq
            part[g, :, c] = dq.astype(BF16)
        pl.when(has2)(lambda: p_partner(g).start())
        for d in range(hn):
            pl.when(hasa)(lambda d=d: p_ahead(g, d).start())
            if d:
                p_own(g, d).start()

    def combine(g):
        @pl.when(has2)
        def _():
            p_partner(g).wait_recv()
            both = own[g, 2 * qb:3 * qb, :] + got[g].astype(F32)
            part[g, 2 * qb:3 * qb, :] = both.astype(BF16)
            for d in range(hn):
                p_two(g, d).start()

    def finish(g):
        for d in range(hn):
            hs = lax.rem(hd + d, hn)
            total = mate[0, hs, g].astype(F32) if d else own[g, pl.ds(piece(hd), rows_out), :]
            total = total + jnp.where(toc, mate[1, hs, g].astype(F32), 0.0)
            total = total + jnp.where(to2, mate[2, hs, g].astype(F32), 0.0)
            outb[:, pl.ds(pl.multiple_of(hs * feats + g * w, w), w)] = total.astype(BF16)

    for g in range(min(AHEAD, chunks)):
        forward(g)
    relay(0)

    @pl.when(has2)
    def _():
        st_two.wait_recv()
        st_relay.start()

    pl.when(hasa)(lambda: st_near.wait_recv())
    pl.when(has2)(lambda: st_relay.wait_recv())
    for o in range(STEPS):
        lse[:, o * qb:(o + 1) * qb] = st[o, :, 0:qb]
        dlt[:, o * qb:(o + 1) * qb] = st[o, :, qb:2 * qb]

    def sent(t):
        low = jnp.where(me + 4 < n, jnp.clip((t - WAIT0) * RATE0, 0, t - LAG0), t - LAG0)
        high = jnp.clip((t - WAIT1) * RATE1, 0, t - LAG1)
        return jnp.clip(jnp.where(quad < 2, low, high), 0, chunks)

    pl.semaphore_wait(ready, hn - 1)
    load_k.wait()
    load_v.wait()

    @pl.loop(1, chunks + 1)
    def _(t):
        pl.when(t < chunks)(lambda: relay(t))
        pl.when(t + AHEAD - 1 < chunks)(lambda: forward(t + AHEAD - 1))
        compute(t - 1)

        @pl.loop(sent(t - 1), sent(t))
        def _(g):
            combine(g)

    @pl.loop(sent(chunks), chunks)
    def _(g):
        combine(g)

    sent_x = x.at[:, :, pl.ds(0, qb)]
    pl.when(q2 | q3 | lower)(lambda: drain(sent_x, xs.at[0]))
    pl.when(odd | lower)(lambda: drain(sent_x, xs.at[1]))
    pl.when(has2)(lambda: drain(x.at[:, :, rows(2)], xs.at[2]))
    if upto > start:
        pl.when(q3 & lower)(lambda: drain(via.at[pl.ds(start, upto - start)], xs.at[3]))
    pl.when(has2)(lambda: drain(part.at[:, rows(oc)], ps))
    pl.when(to2)(lambda: st_two.wait_send())
    pl.when(toc)(lambda: st_near.wait_send())
    pl.when(has2)(lambda: st_relay.wait_send())

    for d in range(hn):
        hs = lax.rem(hd + d, hn)
        if d:
            drain(part.at[:, pl.ds(0, rows_out)], rsnd.at[0, d])
            drain(mate.at[0, hs], rrcv.at[0, hs])
        pl.when(hasa)(lambda d=d: drain(part.at[:, pl.ds(0, rows_out)], rsnd.at[1, d]))
        pl.when(toc)(lambda hs=hs: drain(mate.at[1, hs], rrcv.at[1, hs]))
        if bulk:
            pl.when(to2)(lambda hs=hs: drain(mate.at[2, hs, pl.ds(0, bulk)], rrcv.at[2, hs]))

    @pl.loop(0, bulk)
    def _(g):
        finish(g)

    for g in range(bulk, chunks):
        for hs in range(hn):
            pl.when(to2)(lambda g=g, hs=hs: drain(mate.at[2, hs, g], rrcv.at[order(2, g), hs]))
        finish(g)

    for d in range(hn):
        pl.when(has2)(lambda d=d: drain(part.at[:, pl.ds(0, rows_out)], rsnd.at[2, d]))


def write_out(kgb, vgb, outb, kg_hbm, vg_hbm, qg_hbm, sem):
    copies = [
        pltpu.make_async_copy(src, dst, sem.at[i])
        for i, (src, dst) in enumerate(((kgb, kg_hbm), (vgb, vg_hbm), (outb, qg_hbm)))
    ]
    for copy in copies:
        copy.start()
    for copy in copies:
        copy.wait()


def per_device(query, query_offset, attn_out, out_grad, log_norm, keys, values):
    n = lax.axis_size("seq")
    hn = lax.axis_size("head")
    heads = log_norm.shape[0]
    qb, feats = query.shape
    kbr = keys.shape[0]
    dh = feats // heads
    hc = HEADS_PER_CHUNK
    while heads % hc:
        hc -= 1
    chunks = heads // hc
    w = hc * dh
    dims = (n, hn, heads, hc, dh, qb, kbr)
    span = STEPS * qb
    dma = pltpu.SemaphoreType.DMA
    args = (query, query_offset.reshape(1, qb), attn_out, out_grad, log_norm, keys, values)
    outs = (
        jax.ShapeDtypeStruct((kbr, feats), BF16),
        jax.ShapeDtypeStruct((kbr, feats), BF16),
        jax.ShapeDtypeStruct((qb // hn, feats * hn), BF16),
    )
    grads = pl.pallas_call(
        functools.partial(kernel, dims),
        out_shape=tuple(pltpu.VMEM(o.shape, o.dtype) for o in outs),
        in_specs=[pl.BlockSpec(memory_space=pl.ANY)] * 7,
        out_specs=tuple([pl.BlockSpec(memory_space=pltpu.VMEM)] * 3),
        scratch_shapes=[
            pltpu.VMEM((chunks, 2, span, w), BF16),
            pltpu.VMEM((chunks, 2, qb, w), BF16),
            pltpu.VMEM((kbr, feats), BF16),
            pltpu.VMEM((kbr, feats), BF16),
            pltpu.VMEM((qb, feats), BF16),
            pltpu.VMEM((heads, qb), F32),
            pltpu.VMEM((1, qb), jnp.int32),
            pltpu.VMEM((STEPS, heads, 2 * qb), F32),
            pltpu.VMEM((heads, span), F32),
            pltpu.VMEM((heads, span), F32),
            pltpu.VMEM((1, span), jnp.int32),
            pltpu.VMEM((chunks, span, w), F32),
            pltpu.VMEM((chunks, span, w), BF16),
            pltpu.VMEM((chunks, qb, w), BF16),
            pltpu.VMEM((3, hn, chunks, qb // hn, w), BF16),
            pltpu.VMEM((hc, kbr, span), BF16),
            pltpu.VMEM((hc, kbr, span), BF16),
            dma((6,)), dma((4,)), dma((4, chunks)), dma((3,)), dma((3,)),
            dma(()), dma((chunks,)), dma((3, hn)), dma((5, hn)), pltpu.SemaphoreType.REGULAR,
        ],
        compiler_params=pltpu.CompilerParams(
            collective_id=0, has_side_effects=True, vmem_limit_bytes=40 * 1024 * 1024
        ),
    )(*[pltpu.with_memory_space_constraint(a, pltpu.HBM) for a in args])
    return pl.pallas_call(
        write_out,
        out_shape=outs,
        in_specs=[pl.BlockSpec(memory_space=pltpu.VMEM)] * 3,
        out_specs=tuple([pl.BlockSpec(memory_space=pl.ANY)] * 3),
        scratch_shapes=[dma((3,))],
        compiler_params=pltpu.CompilerParams(vmem_limit_bytes=16 * 1024 * 1024),
    )(*grads)


def solution(mesh):
    in_specs = (
        P("seq", "head"),
        P("seq"),
        P("seq", "head"),
        P("seq", "head"),
        P("head", "seq"),
        P("seq", "head"),
        P("seq", "head"),
    )
    out_specs = (P("seq", "head"), P("seq", "head"), P(("seq", "head"), None))
    return jax.shard_map(
        per_device, mesh=mesh, in_specs=in_specs, out_specs=out_specs, check_vma=False
    )
```

```python
import functools
import math

import jax
import jax.numpy as jnp
from jax import lax
from jax.experimental import pallas as pl
from jax.experimental.pallas import tpu as pltpu
from jax.sharding import PartitionSpec as P

STEPS = 4
HEADS_PER_CHUNK = 2
LAG0 = 1
LAG1 = 1
WAIT1 = 2
RATE1 = 3
WAIT0 = 6
RATE0 = 3
FROM = 2
UPTO = 8
AHEAD = 3
F32 = jnp.float32
BF16 = jnp.bfloat16


def dot(a, b, ca, cb):
    return lax.dot_general(a, b, (((ca,), (cb,)), ((), ())), preferred_element_type=F32)


def kernel(
    dims, q_hbm, off_hbm, o_hbm, do_hbm, ln_hbm, k_hbm, v_hbm,
    kgb, vgb, outb,
    x, via, kb, vb, ob, lnb, offb, st, lse, dlt, offrow, own, part, got, mate, pb, db,
    small_sem, xs, xr, ss, sr, ps, pr, rsnd, rrcv, ready,
):
    n, hn, heads, hc, dh, qb, kbr = dims
    chunks = heads // hc
    w = hc * dh
    feats = heads * dh
    rows_out = qb // hn
    scale = 1.0 / math.sqrt(dh)
    me = lax.axis_index("seq")
    hd = lax.axis_index("head")
    k = lax.rem(me, 2)
    partner = me + 1 - 2 * k
    oa = 1 + 2 * k
    oc = 3 - 2 * k
    quad = lax.rem(me, 4)
    q0, q1, q2, q3 = (quad == i for i in range(4))
    odd = k == 1
    lower = me >= 4
    has2 = me + 2 < n
    hasa = me + oa < n
    to2 = me >= 2
    toc = me >= oc

    def drain(ref, sem):
        pltpu.make_async_copy(ref, ref, sem).wait()

    def rows(o):
        return pl.ds(pl.multiple_of(o * qb, qb), qb)

    def cols(g):
        return pl.ds(pl.multiple_of(g * w, w), w)

    def load_q(g):
        return pltpu.make_async_copy(q_hbm.at[:, cols(g)], x.at[g, 0, pl.ds(0, qb)], small_sem.at[3])

    def load_do(g):
        return pltpu.make_async_copy(do_hbm.at[:, cols(g)], x.at[g, 1, pl.ds(0, qb)], small_sem.at[3])

    load_k = pltpu.make_async_copy(k_hbm, kb, small_sem.at[4])
    load_v = pltpu.make_async_copy(v_hbm, vb, small_sem.at[5])
    load_o = pltpu.make_async_copy(o_hbm, ob, small_sem.at[0])
    load_ln = pltpu.make_async_copy(ln_hbm, lnb, small_sem.at[1])
    load_off = pltpu.make_async_copy(off_hbm, offb, small_sem.at[2])

    def remote(src, dst, send, recv, target):
        return pltpu.make_async_remote_copy(
            src_ref=src, dst_ref=dst, send_sem=send, recv_sem=recv,
            device_id={"seq": target}, device_id_type=pl.DeviceIdType.MESH,
        )

    def mine(g):
        return x.at[g, :, pl.ds(0, qb)]

    def slot(g, o):
        return x.at[g, :, rows(o)]

    def x_two(g):
        return remote(mine(g), slot(g, 2), xs.at[0], xr.at[0, g], me - 2)

    def x_chip(g):
        return remote(mine(g), slot(g, 1), xs.at[1], xr.at[1, g], me - 1)

    def x_three(g):
        return remote(mine(g), slot(g, 3), xs.at[1], xr.at[1, g], me - 3)

    def x_side(g):
        return remote(mine(g), via.at[g], xs.at[0], xr.at[3, g], me + 3)

    def via_down(g):
        return remote(via.at[g], slot(g, 2), xs.at[3], xr.at[0, g], me - 5)

    start = chunks * FROM // 10
    upto = chunks * UPTO // 10

    def relayed(g):
        return (g >= start) & (g < upto)

    def x_relay(g):
        return remote(slot(g, 2), slot(g, oa), xs.at[2], xr.at[2, g], partner)

    st_two = remote(st.at[0], st.at[2], ss.at[0], sr.at[0], me - 2)
    st_near = remote(st.at[0], st.at[oc], ss.at[1], sr.at[1], me - oc)
    st_relay = remote(st.at[2], st.at[oa], ss.at[2], sr.at[2], partner)

    def p_partner(g):
        return remote(part.at[g, rows(oc)], got.at[g], ps, pr.at[g], partner)

    def piece(hs):
        return pl.multiple_of(hs * rows_out, rows_out)

    def back(kind, g, d, ahead, o):
        peer = lax.rem(hd + d, hn)
        return pltpu.make_async_remote_copy(
            src_ref=part.at[g, pl.ds(pl.multiple_of(o * qb, qb) + piece(peer), rows_out)],
            dst_ref=mate.at[kind, hd, g], send_sem=rsnd.at[kind, d], recv_sem=rrcv.at[order(kind, g), hd],
            device_id={"seq": me + ahead, "head": peer}, device_id_type=pl.DeviceIdType.MESH,
        )

    def p_own(g, d):
        return back(0, g, d, 0, 0)

    def p_ahead(g, d):
        return back(1, g, d, oa, oa)

    def p_two(g, d):
        return back(2, g, d, 2, 2)

    bulk = max(chunks - 2, 0)

    def order(kind, g):
        return kind + jnp.maximum(g - bulk + 1, 0) if kind == 2 else kind

    barrier = pltpu.get_barrier_semaphore()

    def greet(cond, ahead, d=0):
        @pl.when(cond)
        def _():
            pl.semaphore_signal(
                barrier, inc=1, device_id={"seq": me + ahead, "head": lax.rem(hd + d, hn)},
                device_id_type=pl.DeviceIdType.MESH,
            )

        return cond.astype(jnp.int32)

    peers = 0
    for o in range(1, STEPS):
        peers = peers + greet(me >= o, -o) + greet(me + o < n, o)
    peers = peers + greet(q3 & lower, -5) + greet(q2 & (me + 5 < n), 5)
    for d in range(1, hn):
        peers = peers + greet(me >= 0, 0, d)

    @pl.loop(0, chunks)
    def _(g):
        load_do(g).start()
        load_q(g).start()

    load_o.start()
    load_ln.start()
    load_off.start()

    drain(x.at[:, :, pl.ds(0, qb)], small_sem.at[3])

    pl.semaphore_wait(barrier, peers)
    for d in range(1, hn):
        pl.semaphore_signal(
            ready, inc=1, device_id={"head": lax.rem(hd + d, hn)}, device_id_type=pl.DeviceIdType.MESH
        )

    def send_x(g):
        pl.when(q2 | q3 | (lower & (q1 | (q0 & jnp.logical_not(relayed(g))))))(lambda: x_two(g).start())
        pl.when(q0 & lower & relayed(g))(lambda: x_side(g).start())
        pl.when(odd)(lambda: x_chip(g).start())
        pl.when((q0 | q2) & lower)(lambda: x_three(g).start())

    send_x(0)

    load_o.wait()
    load_ln.wait()

    st[0, :, 0:qb] = lnb[...]
    eye = lax.broadcasted_iota(jnp.int32, (qb, qb), 0) == lax.broadcasted_iota(jnp.int32, (qb, qb), 1)
    for h in range(heads):
        oh = ob[:, h * dh:(h + 1) * dh]
        doh = x[h // hc, 1, 0:qb, h % hc * dh:(h % hc + 1) * dh]
        t = dot(oh, doh, 1, 1)
        st[0, h:h + 1, qb:2 * qb] = jnp.sum(jnp.where(eye, t, 0.0), axis=0, keepdims=True)

    pl.when(to2)(lambda: st_two.start())
    pl.when(toc)(lambda: st_near.start())

    @pl.loop(1, chunks)
    def _(g):
        send_x(g)

    load_k.start()
    load_v.start()

    for o in range(1, STEPS):

        @pl.when(me + o >= n)
        def _(o=o):
            @pl.loop(0, chunks)
            def _(g):
                for i in range(2):
                    x[g, i, rows(o), :] = jnp.zeros((qb, w), BF16)

            st[o] = jnp.zeros_like(st[o])

    load_off.wait()
    offrow[...] = jnp.full(offrow.shape, kbr, jnp.int32)
    offrow[:, 0:qb] = offb[...]

    def forward(g):
        @pl.when(q3 & lower & relayed(g))
        def _():
            x_side(g).wait_recv()
            via_down(g).start()

    def relay(g):
        @pl.when(has2)
        def _():
            x_two(g).wait_recv()
            x_relay(g).start()

    def compute(g):
        @pl.when(hasa)
        def _():
            x_chip(g).wait_recv()

        pl.when(has2)(lambda: x_relay(g).wait_recv())
        half = 2 * qb
        allowed = lax.broadcasted_iota(jnp.int32, (kbr, half), 0) <= offrow[:, 0:half]
        for h in range(hc):
            c = slice(h * dh, (h + 1) * dh)
            out = pl.ds(pl.multiple_of(g * w + h * dh, dh), dh)
            row = pl.ds(g * hc + h, 1)
            s = dot(kb[:, out], x[g, 0, :, c], 1, 1) * scale - lse[row, :]
            p = jnp.exp(s)
            p = jnp.concatenate([jnp.where(allowed, p[:, 0:half], 0.0), p[:, half:]], axis=1)
            pb[h] = p.astype(BF16)
            dp = dot(vb[:, out], x[g, 1, :, c], 1, 1)
            db[h] = (p * (dp - dlt[row, :]) * scale).astype(BF16)
        for h in range(hc):
            c = slice(h * dh, (h + 1) * dh)
            out = pl.ds(pl.multiple_of(g * w + h * dh, dh), dh)
            vgb[:, out] = dot(pb[h], x[g, 1, :, c], 1, 0).astype(BF16)
            kgb[:, out] = dot(db[h], x[g, 0, :, c], 1, 0).astype(BF16)
            dq = dot(db[h], kb[:, out], 0, 0)
            own[g, :, c] = dq
            part[g, :, c] = dq.astype(BF16)
        pl.when(has2)(lambda: p_partner(g).start())
        for d in reversed(range(hn)):
            pl.when(hasa)(lambda d=d: p_ahead(g, d).start())
            if d:
                p_own(g, d).start()

    def combine(g):
        @pl.when(has2)
        def _():
            p_partner(g).wait_recv()
            both = own[g, 2 * qb:3 * qb, :] + got[g].astype(F32)
            part[g, 2 * qb:3 * qb, :] = both.astype(BF16)
            for d in reversed(range(hn)):
                p_two(g, d).start()

    def finish(g):
        for d in range(hn):
            hs = lax.rem(hd + d, hn)
            total = mate[0, hs, g].astype(F32) if d else own[g, pl.ds(piece(hd), rows_out), :]
            total = total + jnp.where(toc, mate[1, hs, g].astype(F32), 0.0)
            total = total + jnp.where(to2, mate[2, hs, g].astype(F32), 0.0)
            outb[:, pl.ds(pl.multiple_of(hs * feats + g * w, w), w)] = total.astype(BF16)

    for g in range(min(AHEAD, chunks)):
        forward(g)
    relay(0)

    @pl.when(has2)
    def _():
        st_two.wait_recv()
        st_relay.start()

    pl.when(hasa)(lambda: st_near.wait_recv())
    pl.when(has2)(lambda: st_relay.wait_recv())
    for o in range(STEPS):
        lse[:, o * qb:(o + 1) * qb] = st[o, :, 0:qb]
        dlt[:, o * qb:(o + 1) * qb] = st[o, :, qb:2 * qb]

    def sent(t):
        low = jnp.where(me + 4 < n, jnp.clip((t - WAIT0) * RATE0, 0, t - LAG0), t - LAG0)
        high = jnp.clip((t - WAIT1) * RATE1, 0, t - LAG1)
        return jnp.clip(jnp.where(quad < 2, low, high), 0, chunks)

    pl.semaphore_wait(ready, hn - 1)
    load_k.wait()
    load_v.wait()

    @pl.loop(1, chunks + 1)
    def _(t):
        pl.when(t < chunks)(lambda: relay(t))
        pl.when(t + AHEAD - 1 < chunks)(lambda: forward(t + AHEAD - 1))
        compute(t - 1)

        @pl.loop(sent(t - 1), sent(t))
        def _(g):
            combine(g)

    @pl.loop(sent(chunks), chunks)
    def _(g):
        combine(g)

    sent_x = x.at[:, :, pl.ds(0, qb)]
    pl.when(q2 | q3 | lower)(lambda: drain(sent_x, xs.at[0]))
    pl.when(odd | lower)(lambda: drain(sent_x, xs.at[1]))
    pl.when(has2)(lambda: drain(x.at[:, :, rows(2)], xs.at[2]))
    if upto > start:
        pl.when(q3 & lower)(lambda: drain(via.at[pl.ds(start, upto - start)], xs.at[3]))
    pl.when(has2)(lambda: drain(part.at[:, rows(oc)], ps))
    pl.when(to2)(lambda: st_two.wait_send())
    pl.when(toc)(lambda: st_near.wait_send())
    pl.when(has2)(lambda: st_relay.wait_send())

    for d in range(hn):
        hs = lax.rem(hd + d, hn)
        if d:
            drain(part.at[:, pl.ds(0, rows_out)], rsnd.at[0, d])
            drain(mate.at[0, hs], rrcv.at[0, hs])
        pl.when(hasa)(lambda d=d: drain(part.at[:, pl.ds(0, rows_out)], rsnd.at[1, d]))
        pl.when(toc)(lambda hs=hs: drain(mate.at[1, hs], rrcv.at[1, hs]))
        if bulk:
            pl.when(to2)(lambda hs=hs: drain(mate.at[2, hs, pl.ds(0, bulk)], rrcv.at[2, hs]))

    @pl.loop(0, bulk)
    def _(g):
        finish(g)

    for g in range(bulk, chunks):
        for hs in range(hn):
            pl.when(to2)(lambda g=g, hs=hs: drain(mate.at[2, hs, g], rrcv.at[order(2, g), hs]))
        finish(g)

    for d in range(hn):
        pl.when(has2)(lambda d=d: drain(part.at[:, pl.ds(0, rows_out)], rsnd.at[2, d]))


def write_out(kgb, vgb, outb, kg_hbm, vg_hbm, qg_hbm, sem):
    copies = [
        pltpu.make_async_copy(src, dst, sem.at[i])
        for i, (src, dst) in enumerate(((kgb, kg_hbm), (vgb, vg_hbm), (outb, qg_hbm)))
    ]
    for copy in copies:
        copy.start()
    for copy in copies:
        copy.wait()


def per_device(query, query_offset, attn_out, out_grad, log_norm, keys, values):
    n = lax.axis_size("seq")
    hn = lax.axis_size("head")
    heads = log_norm.shape[0]
    qb, feats = query.shape
    kbr = keys.shape[0]
    dh = feats // heads
    hc = HEADS_PER_CHUNK
    while heads % hc:
        hc -= 1
    chunks = heads // hc
    w = hc * dh
    dims = (n, hn, heads, hc, dh, qb, kbr)
    span = STEPS * qb
    dma = pltpu.SemaphoreType.DMA
    args = (query, query_offset.reshape(1, qb), attn_out, out_grad, log_norm, keys, values)
    outs = (
        jax.ShapeDtypeStruct((kbr, feats), BF16),
        jax.ShapeDtypeStruct((kbr, feats), BF16),
        jax.ShapeDtypeStruct((qb // hn, feats * hn), BF16),
    )
    grads = pl.pallas_call(
        functools.partial(kernel, dims),
        out_shape=tuple(pltpu.VMEM(o.shape, o.dtype) for o in outs),
        in_specs=[pl.BlockSpec(memory_space=pl.ANY)] * 7,
        out_specs=tuple([pl.BlockSpec(memory_space=pltpu.VMEM)] * 3),
        scratch_shapes=[
            pltpu.VMEM((chunks, 2, span, w), BF16),
            pltpu.VMEM((chunks, 2, qb, w), BF16),
            pltpu.VMEM((kbr, feats), BF16),
            pltpu.VMEM((kbr, feats), BF16),
            pltpu.VMEM((qb, feats), BF16),
            pltpu.VMEM((heads, qb), F32),
            pltpu.VMEM((1, qb), jnp.int32),
            pltpu.VMEM((STEPS, heads, 2 * qb), F32),
            pltpu.VMEM((heads, span), F32),
            pltpu.VMEM((heads, span), F32),
            pltpu.VMEM((1, span), jnp.int32),
            pltpu.VMEM((chunks, span, w), F32),
            pltpu.VMEM((chunks, span, w), BF16),
            pltpu.VMEM((chunks, qb, w), BF16),
            pltpu.VMEM((3, hn, chunks, qb // hn, w), BF16),
            pltpu.VMEM((hc, kbr, span), BF16),
            pltpu.VMEM((hc, kbr, span), BF16),
            dma((6,)), dma((4,)), dma((4, chunks)), dma((3,)), dma((3,)),
            dma(()), dma((chunks,)), dma((3, hn)), dma((5, hn)), pltpu.SemaphoreType.REGULAR,
        ],
        compiler_params=pltpu.CompilerParams(
            collective_id=0, has_side_effects=True, vmem_limit_bytes=40 * 1024 * 1024
        ),
    )(*[pltpu.with_memory_space_constraint(a, pltpu.HBM) for a in args])
    return pl.pallas_call(
        write_out,
        out_shape=outs,
        in_specs=[pl.BlockSpec(memory_space=pltpu.VMEM)] * 3,
        out_specs=tuple([pl.BlockSpec(memory_space=pl.ANY)] * 3),
        scratch_shapes=[dma((3,))],
        compiler_params=pltpu.CompilerParams(vmem_limit_bytes=16 * 1024 * 1024),
    )(*grads)


def solution(mesh):
    in_specs = (
        P("seq", "head"),
        P("seq"),
        P("seq", "head"),
        P("seq", "head"),
        P("head", "seq"),
        P("seq", "head"),
        P("seq", "head"),
    )
    out_specs = (P("seq", "head"), P("seq", "head"), P(("seq", "head"), None))
    return jax.shard_map(
        per_device, mesh=mesh, in_specs=in_specs, out_specs=out_specs, check_vma=False
    )
```
